32 devices in a mesh: dp: 4 (over y, x), owner: 8 (over z, core).
Axes of the slice: x: 2, y: 2, z: 4, core: 2. Of those that a mesh axis runs over, the one named last changes fastest.
Arguments:
- partial_grads: bfloat16 [4, 48, 1024, 1024], P('dp', None, 'owner'), may hold values from -2.09375 to 2.09375
- owner_map: int32 [48], replicated, may hold values from 0 to 7, as said below
- left_stats: float32 [8, 12, 1024, 1024], P('owner', None, 'dp'), may hold values from -1.8 to 1.8
- right_stats: float32 [8, 12, 1024, 1024], P('owner', None, 'dp'), may hold values from -1.8 to 1.8
- left_roots: bfloat16 [8, 12, 1024, 1024], P('owner', None, 'dp'), as said below
- right_roots: bfloat16 [8, 12, 1024, 1024], P('owner', None, 'dp'), as said below
Outputs:
- direction: bfloat16 [48, 1024, 1024], P(None, ('dp', 'owner'))
- new_left_stats: float32 [8, 12, 1024, 1024], P('owner', None, 'dp')
- new_right_stats: float32 [8, 12, 1024, 1024], P('owner', None, 'dp')
The draws below stay inside these ranges and needn't reach their ends.
Inputs may be any that keep to these rules, and one draw needn't show every extreme that they name: `owner_map`: no owner index holds more than 12 blocks, and some owner holds exactly 12. `left_roots`: each block is dense and not symmetric; its diagonal entries are of order one and its off-diagonal entries are small. `right_roots`: each block is dense and not symmetric; its diagonal entries are of order one and its off-diagonal entries are small.
All inputs are finite; a program needn't handle non-finite values.
Results may differ from the reference program's by a relative error of at most 0.017.
Values may be sent and summed in bfloat16 or wider, within the bound.
A program may use at most 256 MiB of HBM per device.

```python
import jax
import jax.numpy as jnp
from jax import lax

D_MODEL = 2560
D_IN = 10576
D_INNER = 5120
TILE = 1024
TILES = 48
OWNERS = 8
SLOTS = 12
N_DP = 4


def draw_owner_map(key, part):
    first, second = jax.random.split(jax.random.fold_in(key, 7))
    total = OWNERS * SLOTS
    ranks = jax.random.permutation(first, total).astype(jnp.int32)
    chosen = jax.random.randint(second, (), 0, OWNERS, dtype=jnp.int32)
    ids = jnp.arange(total, dtype=jnp.int32)
    keyed = jnp.where(ids // SLOTS == chosen, -1 - ids % SLOTS, ranks)
    order = jnp.argsort(keyed, stable=True).astype(jnp.int32)
    return (order[:TILES] // SLOTS).astype(jnp.int32)


def draw_root(key):
    first, second = jax.random.split(key)
    shape = (OWNERS, SLOTS, TILE, TILE)
    diag = jax.random.uniform(first, (OWNERS, SLOTS, TILE), jnp.float32, 0.5, 1.5)
    off = jax.random.normal(second, shape, jnp.float32) * (0.4 / TILE ** 0.5)
    eye = jnp.eye(TILE, dtype=jnp.float32)
    return off + diag[..., None] * eye


def draw_left_roots(key, part):
    return draw_root(jax.random.fold_in(key, 11)).astype(jnp.bfloat16)


def draw_right_roots(key, part):
    return draw_root(jax.random.fold_in(key, 13)).astype(jnp.bfloat16)


def shard_levels(own_key, shape, shards, least, high):
    level = 1.0
    for position, shards_of in shards:
        draws = jax.random.uniform(jax.random.fold_in(jax.random.fold_in(own_key, 6), position), (shards_of,), jnp.float32, least / len(shards), high / len(shards))
        level = level * jnp.repeat(jnp.exp(draws), shape[position] // shards_of).reshape((-1,) + (1,) * (len(shape) - 1 - position))
    return level


def centred(key, shape, deviation, limit, shards=(), kind=jnp.bfloat16):
    values = deviation * jax.random.normal(key, shape, jnp.float32)
    if shards:
        values = values * shard_levels(key, shape, shards, -0.22, 0.18)
    return jnp.clip(values, -limit, limit).astype(kind)


def setup_inputs(seed: int = 0) -> dict:
    key_of = jax.random.split(jax.random.key(seed), 7)
    partial_grads = centred(key_of[0], (N_DP, TILES, TILE, TILE), 0.35, 2.09375, ((0, 4), (2, 8)))
    owner_map = draw_owner_map(jax.random.fold_in(key_of[6], 71), 0)
    left_stats = centred(key_of[2], (OWNERS, SLOTS, TILE, TILE), 0.3, 1.8, ((0, 8), (2, 4)), jnp.float32)
    right_stats = centred(key_of[3], (OWNERS, SLOTS, TILE, TILE), 0.3, 1.8, ((0, 8), (2, 4)), jnp.float32)
    left_roots = draw_left_roots(jax.random.fold_in(key_of[6], 71), 0)
    right_roots = draw_right_roots(jax.random.fold_in(key_of[6], 71), 0)
    return {"partial_grads": partial_grads, "owner_map": owner_map, "left_stats": left_stats, "right_stats": right_stats, "left_roots": left_roots, "right_roots": right_roots}


stat_decay = 0.999


def extents(count):
    index = jnp.arange(count, dtype=jnp.int32)
    in_cols = -(-D_IN // TILE)
    out_cols = -(-D_MODEL // TILE)
    in_count = (-(-D_MODEL // TILE)) * in_cols
    is_in = index < in_count
    other = jnp.maximum(index - in_count, 0)
    rows = jnp.where(is_in, jnp.minimum(TILE, D_MODEL - (index // in_cols) * TILE), jnp.minimum(TILE, D_INNER - (other // out_cols) * TILE))
    cols = jnp.where(is_in, jnp.minimum(TILE, D_IN - (index % in_cols) * TILE), jnp.minimum(TILE, D_MODEL - (other % out_cols) * TILE))
    return rows.astype(jnp.int32), cols.astype(jnp.int32)


def reference(partial_grads, owner_map, left_stats, right_stats, left_roots, right_roots):
    rows, cols = extents(TILES)
    line = jnp.arange(TILE, dtype=jnp.int32)
    mask = (line[None, :, None] < rows[:, None, None]) & (line[None, None, :] < cols[:, None, None])
    total = jnp.zeros(partial_grads.shape[1:], jnp.float32)
    for source in range(N_DP):
        total = total + partial_grads[source].astype(jnp.float32)
    grads = jnp.where(mask, total, jnp.float32(0.0)).astype(jnp.bfloat16)
    ids = jnp.arange(TILES, dtype=jnp.int32)
    same = (owner_map[:, None] == owner_map[None, :]) & (ids[None, :] < ids[:, None])
    slot = jnp.sum(same.astype(jnp.int32), axis=1).astype(jnp.int32)

    def per_tile(index):
        grad = grads[index]
        owner = owner_map[index]
        place = slot[index]
        left_new = stat_decay * left_stats[owner, place] + (1.0 - stat_decay) * jnp.dot(grad, grad.T, preferred_element_type=jnp.float32)
        right_new = stat_decay * right_stats[owner, place] + (1.0 - stat_decay) * jnp.dot(grad.T, grad, preferred_element_type=jnp.float32)
        left_part = jnp.dot(left_roots[owner, place], grad, preferred_element_type=jnp.float32).astype(jnp.bfloat16)
        result = jnp.dot(left_part, right_roots[owner, place], preferred_element_type=jnp.float32)
        result = jnp.where(mask[index], result, jnp.float32(0.0)).astype(jnp.bfloat16)
        return left_new, right_new, result

    left_all, right_all, direction = lax.map(per_tile, ids)
    new_left = (stat_decay * left_stats).at[owner_map, slot].set(left_all)
    new_right = (stat_decay * right_stats).at[owner_map, slot].set(right_all)
    return (direction, new_left, new_right)
```

```python
import functools

import jax
import jax.numpy as jnp
from jax import lax
from jax.experimental import pallas as pl
from jax.experimental.pallas import tpu as pltpu
from jax.sharding import PartitionSpec as P


D_MODEL = 2560
D_IN = 10576
D_INNER = 5120
TILE = 1024

stat_decay = 0.999


def extents(count):
    index = jnp.arange(count, dtype=jnp.int32)
    in_cols = -(-D_IN // TILE)
    out_cols = -(-D_MODEL // TILE)
    in_count = -(-D_MODEL // TILE) * in_cols
    is_in = index < in_count
    other = jnp.maximum(index - in_count, 0)
    rows = jnp.where(
        is_in,
        jnp.minimum(TILE, D_MODEL - index // in_cols * TILE),
        jnp.minimum(TILE, D_INNER - other // out_cols * TILE),
    )
    cols = jnp.where(
        is_in,
        jnp.minimum(TILE, D_IN - index % in_cols * TILE),
        jnp.minimum(TILE, D_MODEL - other % out_cols * TILE),
    )
    return (rows, cols)


def dot(a, b, dims):
    return lax.dot_general(a, b, (dims, ((), ())), preferred_element_type=jnp.float32)


def step_kernel(base, info, grads, roots, left_roots, left_stats, right_stats, *rest):
    direction, new_left, new_right, left_part = rest[-4:]
    dp, _, _, piece, width = grads.shape
    lanes, tile = left_stats.shape[1:]
    here = info[0]
    pieces = lanes // piece
    full = [grads[d].reshape(tile, width) for d in range(dp)]
    mine = grads[here].reshape(tile, width).T
    gram = None
    for d in range(dp):
        right = dot(mine, full[d], ((1,), (0,)))
        cut = (0, slice(None), slice(d * width, (d + 1) * width))
        new_right[cut] = stat_decay * right_stats[cut] + (1.0 - stat_decay) * right
        part = dot(left_roots[0], full[d], ((1,), (0,)))
        left_part[:, d * width : (d + 1) * width] = part.astype(jnp.bfloat16)
        rows = grads[d, pl.ds(here * pieces, pieces)].reshape(lanes, width)
        term = dot(rows, full[d], ((1,), (1,)))
        gram = term if gram is None else gram + term
    new_left[0] = stat_decay * left_stats[0] + (1.0 - stat_decay) * gram
    product = dot(left_part[...], roots[...].reshape(tile, tile), ((1,), (0,)))
    slot = base + pl.program_id(0)
    row = lax.broadcasted_iota(jnp.int32, product.shape, 0)
    col = lax.broadcasted_iota(jnp.int32, product.shape, 1)
    keep = (row < info[1 + 2 * slot]) & (col < info[2 + 2 * slot])
    result = jnp.where(keep, product, 0.0).astype(jnp.bfloat16)
    direction[...] = result.reshape(direction.shape)


def step(base, chunk, info, grads, roots, left_roots, left_stats, right_stats, carried):
    dp, owners, _, piece, width = grads.shape
    _, lanes, tile = left_stats.shape
    at = lambda s, info: (base + s, 0, 0)
    stats = pl.BlockSpec((1, lanes, tile), at)
    in_specs = [
        pl.BlockSpec((dp, owners, 1, piece, width), lambda s, info: (0, 0, s, 0, 0)),
        pl.BlockSpec((dp, 1, lanes, tile), lambda s, info: (0, base + s, 0, 0)),
        stats,
        stats,
        stats,
    ] + [pl.BlockSpec(memory_space=pl.ANY)] * len(carried)
    sub = lanes // owners
    return pl.pallas_call(
        functools.partial(step_kernel, base),
        grid_spec=pltpu.PrefetchScalarGridSpec(
            num_scalar_prefetch=1,
            grid=(chunk,),
            in_specs=in_specs,
            out_specs=[
                pl.BlockSpec((owners, 1, sub, tile), lambda s, info: (0, s, 0, 0)),
                stats,
                stats,
            ],
            scratch_shapes=[pltpu.VMEM((lanes, tile), jnp.bfloat16)],
        ),
        out_shape=[
            jax.ShapeDtypeStruct((owners, chunk, sub, tile), jnp.bfloat16),
            jax.ShapeDtypeStruct(left_stats.shape, jnp.float32),
            jax.ShapeDtypeStruct(right_stats.shape, jnp.float32),
        ],
        input_output_aliases={6: 1, 7: 2} if carried else {},
        compiler_params=pltpu.CompilerParams(vmem_limit_bytes=48 * 1024 * 1024),
        cost_estimate=pl.CostEstimate(
            flops=8 * chunk * lanes * tile * tile,
            bytes_accessed=chunk * (4 * tile * tile + 20 * lanes * tile),
            transcendentals=0,
        ),
    )(info, grads, roots, left_roots, left_stats, right_stats, *carried)


def chunks_of(slots):
    if slots < 6:
        sizes = (slots,)
    else:
        last, middle = slots // 4, slots // 3
        sizes = (slots - middle - last, middle, last)
    return [(sum(sizes[:index]), size) for index, size in enumerate(sizes)]


def general(partial_grads, owner_map, left_stats, right_stats, left_roots, right_roots):
    dp = lax.axis_size("dp")
    owners = lax.axis_size("owner")
    owner_here = lax.axis_index("owner")
    dp_here = lax.axis_index("dp")
    tiles = owner_map.shape[0]
    slots = left_stats.shape[1]
    lanes = left_stats.shape[2]
    tile = left_stats.shape[3]
    piece = partial_grads.shape[2]
    width = tile // dp
    rows, cols = extents(tiles)
    ids = jnp.arange(tiles, dtype=jnp.int32)
    same = (owner_map[:, None] == owner_map[None, :]) & (ids[None, :] < ids[:, None])
    slot = jnp.sum(same.astype(jnp.int32), axis=1)
    picks = (slot[None, None, :] == jnp.arange(slots, dtype=jnp.int32)[None, :, None]) & (
        owner_map[None, None, :] == jnp.arange(owners, dtype=jnp.int32)[:, None, None]
    )
    tile_of = jnp.sum(jnp.where(picks, ids[None, None, :], 0), axis=2)
    filled = jnp.any(picks, axis=2)

    shares = lax.psum_scatter(partial_grads[0], "dp", scatter_dimension=2, tiled=True)
    roots = lax.all_gather(right_roots[0], "dp", axis=0)

    piece_rows = owner_here * piece + jnp.arange(piece, dtype=jnp.int32)
    piece_cols = dp_here * width + jnp.arange(width, dtype=jnp.int32)
    tile_here = lax.dynamic_index_in_dim(tile_of, owner_here, 0, keepdims=False)
    info = jnp.stack([jnp.take(rows, tile_here) - dp_here * lanes, jnp.take(cols, tile_here)], 1)
    info = jnp.concatenate([dp_here[None], info.reshape(-1)]).astype(jnp.int32)

    spans = chunks_of(slots)
    arrived = []
    for base, chunk in spans:
        which = tile_of[:, base : base + chunk]
        rows_of = jnp.where(filled[:, base : base + chunk], jnp.take(rows, which), 0)
        mask = (piece_rows[:, None] < rows_of[:, :, None, None]) & (
            piece_cols[None, :] < jnp.take(cols, which)[:, :, None, None]
        )
        taken = jnp.take(shares, which.reshape(-1), axis=0).reshape(owners, chunk, piece, width)
        sent = lax.all_to_all(
            jnp.where(mask, taken, jnp.zeros((), shares.dtype)),
            "owner",
            split_axis=0,
            concat_axis=0,
            tiled=True,
        )
        arrived.append(sent)

    def place(index, returned, direction):
        base, chunk = spans[index]
        flat = returned.reshape(owners * chunk, lanes // owners, tile)
        inside = (slot >= base) & (slot < base + chunk)
        at = jnp.where(inside, owner_map * chunk + slot - base, 0)
        return jnp.where(inside[:, None, None], jnp.take(flat, at, axis=0), direction)

    direction = jnp.zeros((tiles, lanes // owners, tile), jnp.bfloat16)
    carried = ()
    for index, (base, chunk) in enumerate(spans):
        grads = lax.all_gather(arrived[index], "dp", axis=0)
        if index:
            direction = place(index - 1, returned, direction)
            grads, direction = lax.optimization_barrier((grads, direction))
        result, *carried = step(
            base, chunk, info, grads, roots, left_roots[0], left_stats[0], right_stats[0], carried
        )
        returned = lax.all_to_all(result, "owner", split_axis=0, concat_axis=0, tiled=True)
    direction = place(len(spans) - 1, returned, direction)
    new_left, new_right = carried
    return (direction, new_left[None], new_right[None])


MESH = pl.DeviceIdType.MESH


def owner_slots(owner_map, owners, slots):
    tiles = owner_map.shape[0]
    ids = jnp.arange(tiles, dtype=jnp.int32)
    same = (owner_map[:, None] == owner_map[None, :]) & (ids[None, :] < ids[:, None])
    slot = jnp.sum(same.astype(jnp.int32), axis=1)
    picks = (slot[None, None, :] == jnp.arange(slots, dtype=jnp.int32)[None, :, None]) & (
        owner_map[None, None, :] == jnp.arange(owners, dtype=jnp.int32)[:, None, None]
    )
    tile_of = jnp.sum(jnp.where(picks, ids[None, None, :], 0), axis=2)
    return slot, tile_of, jnp.any(picks, axis=2)


def exchange_kernel(
    counts, sent, roots, left_roots, left_stats, right_stats,
    returned, new_left, new_right, wide,
    g_v, r_v, l_v, ls_v, rs_v, part_v, mine_v, out_v, nl_v, nr_v,
    own_sem, to_send, to_recv, wide_send, wide_recv, back_send, back_recv, back_own,
    g_sem, r_sem, in_sem, nl_sem, nr_sem,
):
    owners, slots, strip, tile = sent.shape
    lanes = left_roots.shape[1]
    parities = len(counts)
    panels = wide.shape[1]
    half = owners // 2
    pieces = lanes // (tile // owners)
    own = lax.axis_index("owner")
    me = lax.axis_index("dp")
    across = me + 1 - 2 * (me % 2)
    along = me + 2 - 4 * (me // 2)
    far = 3 - me
    kind = own % parities
    many = sum(jnp.where(kind == p, counts[p], 0) for p in range(parities))
    others = [(own + j) % owners for j in range(1, owners)]

    barrier = pltpu.get_barrier_semaphore()
    for peer in (across, along):
        pl.semaphore_signal(barrier, inc=1, device_id={"dp": peer}, device_id_type=MESH)
    for peer in others:
        pl.semaphore_signal(barrier, inc=1, device_id={"owner": peer}, device_id_type=MESH)
    pl.semaphore_wait(barrier, owners + 1)

    def each(low, high, act):
        lax.fori_loop(low, high, lambda i, c: (act(i), c)[1], 0)

    def place_of(item):
        return jnp.where(item < many, item, slots + item - many)

    def own_copy(s):
        return pltpu.make_async_copy(
            sent.at[own, s], wide.at[slots + s, me, own], own_sem.at[s]
        )

    def give(s, peer):
        return pltpu.make_async_remote_copy(
            src_ref=sent.at[peer, s],
            dst_ref=wide.at[slots + s, me, own],
            send_sem=to_send.at[peer % parities, s],
            recv_sem=to_recv.at[s],
            device_id={"owner": peer},
            device_id_type=MESH,
        )

    def direct(src, place, axis, peer):
        return pltpu.make_async_remote_copy(
            src_ref=src,
            dst_ref=wide.at[place, me],
            send_sem=wide_send.at[place, axis],
            recv_sem=wide_recv.at[place, axis],
            device_id={"dp": peer},
            device_id_type=MESH,
        )

    def forward(place, axis, panel, first, peer):
        piece = wide.at[place, panel, pl.ds(first, half)]
        return pltpu.make_async_remote_copy(
            src_ref=piece,
            dst_ref=piece,
            send_sem=wide_send.at[place, axis],
            recv_sem=wide_recv.at[place, axis],
            device_id={"dp": peer},
            device_id_type=MESH,
        )

    def sized(ref, sem):
        return pltpu.make_async_copy(ref, ref, sem)

    def loads(s):
        made = [pltpu.make_async_copy(roots.at[s], r_v.at[me], r_sem.at[0])]
        for index, panel in enumerate((across, along, far)):
            made.append(
                pltpu.make_async_copy(wide.at[s, panel], r_v.at[panel], r_sem.at[1 + index])
            )
        made.append(pltpu.make_async_copy(left_roots.at[s], l_v, in_sem.at[0]))
        made.append(pltpu.make_async_copy(left_stats.at[s], ls_v, in_sem.at[1]))
        made.append(pltpu.make_async_copy(right_stats.at[s], rs_v, in_sem.at[2]))
        return made

    def grads(s):
        return [
            pltpu.make_async_copy(wide.at[slots + s, j], g_v.at[:, j], g_sem.at[j])
            for j in range(panels)
        ]

    def back(s, side, peer):
        return pltpu.make_async_remote_copy(
            src_ref=out_v.at[side, peer],
            dst_ref=returned.at[own, s],
            send_sem=back_send.at[side],
            recv_sem=back_recv.at[kind, s],
            device_id={"owner": peer},
            device_id_type=MESH,
        )

    def back_home(s, side):
        return pltpu.make_async_copy(out_v.at[side, own], returned.at[own, s], back_own.at[side])

    def stats_out(s, side):
        return (
            pltpu.make_async_copy(nl_v.at[side], new_left.at[s], nl_sem.at[side]),
            pltpu.make_async_copy(nr_v.at[side], new_right.at[s], nr_sem.at[side]),
        )

    def settle(s, side):
        sized(returned.at[0, pl.ds(0, owners - 1)], back_send.at[side]).wait()
        back_home(s, side).wait()
        for copy in stats_out(s, side):
            copy.wait()

    width = lanes

    def compute(s):
        side = s % 2
        for copy in grads(s):
            copy.start()

        @pl.when(s == 0)
        def _():
            for copy in loads(0):
                copy.start()

        @pl.when(s >= 2)
        def _():
            settle(s - 2, side)

        for copy in grads(s) + loads(s):
            copy.wait()

        def cols(c):
            return pl.ds(pl.multiple_of(c * width, width), width)

        def column(c):
            return g_v[:, :, :, cols(c)].reshape(tile, width)

        def first(c):
            part = dot(l_v[...], column(c), ((1,), (0,)))
            part_v[:, cols(c)] = part.astype(jnp.bfloat16)

        def second(c):
            right = r_v[:, :, :, cols(c)].reshape(tile, width)
            product = dot(part_v[...], right, ((1,), (0,)))
            out_v[side, :, :, cols(c)] = product.astype(jnp.bfloat16).reshape(owners, strip, width)

        each(0, tile // width, first)
        each(0, tile // width, second)
        for peer in others:
            back(s, side, peer).start()
        back_home(s, side).start()
        mine_v[...] = column(me).T

        def third(c):
            right = dot(mine_v[...], column(c), ((1,), (0,)))
            nr_v[side, :, cols(c)] = stat_decay * rs_v[:, cols(c)] + (1.0 - stat_decay) * right
            rows = g_v[pl.ds(me * pieces, pieces)].reshape(lanes, tile)
            block = g_v[pl.ds(c * pieces, pieces)].reshape(lanes, tile)
            left = dot(rows, block, ((1,), (1,)))
            nl_v[side, :, cols(c)] = stat_decay * ls_v[:, cols(c)] + (1.0 - stat_decay) * left

        each(0, tile // width, third)
        for copy in stats_out(s, side):
            copy.start()

        @pl.when(s + 1 < many)
        def _():
            for copy in loads(s + 1):
                copy.start()

    each(0, many, lambda s: own_copy(s).start())

    def turn(i):
        @pl.when(i < many)
        def _():
            direct(roots.at[i], i, 0, across).start()
            direct(roots.at[i], i, 1, along).start()

        @pl.when(i < slots)
        def _():
            for peer in others:
                if min(counts) == slots:
                    give(i, peer).start()
                else:
                    for p in range(parities):
                        @pl.when((peer % parities == p) & (i < counts[p]))
                        def _():
                            give(i, peer).start()

        @pl.when((i >= many) & (i < 2 * many))
        def _():
            s = i - many
            own_copy(s).wait()
            sized(wide.at[slots + s, me, pl.ds(0, owners - 1)], to_recv.at[s]).wait()
            direct(wide.at[slots + s, me], slots + s, 0, across).start()
            direct(wide.at[slots + s, me], slots + s, 1, along).start()

        @pl.when((i >= 1) & (i < 2 * many + 1))
        def _():
            place = place_of(i - 1)
            sized(wide.at[place, across], wide_recv.at[place, 0]).wait()
            forward(place, 2, across, 0, along).start()
            sized(wide.at[place, along], wide_recv.at[place, 1]).wait()
            forward(place, 3, along, half, across).start()

        @pl.when(i >= 2)
        def _():
            place = place_of(i - 2)
            sized(wide.at[place, far, pl.ds(0, half)], wide_recv.at[place, 2]).wait()
            sized(wide.at[place, far, pl.ds(half, half)], wide_recv.at[place, 3]).wait()

        @pl.when(i >= many + 2)
        def _():
            compute(i - 2 - many)

    each(0, 2 * many + 2, turn)

    settle(many - 2, many % 2)
    settle(many - 1, (many + 1) % 2)

    if min(counts) < slots:
        def fade(s):
            moved = [
                pltpu.make_async_copy(left_stats.at[s], ls_v, in_sem.at[1]),
                pltpu.make_async_copy(right_stats.at[s], rs_v, in_sem.at[2]),
            ]
            for copy in moved:
                copy.start()
            for copy in moved:
                copy.wait()
            nl_v[0] = stat_decay * ls_v[...]
            nr_v[0] = stat_decay * rs_v[...]
            for copy in stats_out(s, 0):
                copy.start()
            for copy in stats_out(s, 0):
                copy.wait()

        each(many, slots, fade)

    def sends(item):
        place = place_of(item)
        panel = wide.at[place, me]
        part = wide.at[place, me, pl.ds(0, half)]
        sized(panel, wide_send.at[place, 0]).wait()
        sized(panel, wide_send.at[place, 1]).wait()
        sized(part, wide_send.at[place, 2]).wait()
        sized(part, wide_send.at[place, 3]).wait()

    each(0, 2 * many, sends)
    group = owners // parities
    for p in range(parities):
        def ends(s, p=p):
            for alike in (True, False):
                size = group - 1 if alike else group

                @pl.when((kind == p) == alike)
                def _():
                    piece = sent.at[0, pl.ds(0, size)]
                    sized(piece, to_send.at[p, s]).wait()
                    sized(piece, back_recv.at[p, s]).wait()

        each(0, counts[p], ends)


def exchange(counts, sent, roots, left_roots, left_stats, right_stats):
    owners, slots, strip, tile = sent.shape
    lanes = left_stats.shape[1]
    dp = tile // lanes
    anywhere = pl.BlockSpec(memory_space=pl.ANY)
    bf16, f32 = jnp.bfloat16, jnp.float32
    dma = pltpu.SemaphoreType.DMA
    return pl.pallas_call(
        functools.partial(exchange_kernel, counts),
        in_specs=[pl.BlockSpec(memory_space=pltpu.VMEM)] + [anywhere] * 4,
        out_specs=[anywhere] * 4,
        out_shape=[
            jax.ShapeDtypeStruct((owners, slots, strip, tile), bf16),
            jax.ShapeDtypeStruct(left_stats.shape, f32),
            jax.ShapeDtypeStruct(right_stats.shape, f32),
            jax.ShapeDtypeStruct((2 * slots, dp, owners, strip, tile), bf16),
        ],
        scratch_shapes=[
            pltpu.VMEM((owners, dp, strip, tile), bf16),
            pltpu.VMEM((dp, owners, strip, tile), bf16),
            pltpu.VMEM((lanes, tile), bf16),
            pltpu.VMEM((lanes, tile), f32),
            pltpu.VMEM((lanes, tile), f32),
            pltpu.VMEM((lanes, tile), bf16),
            pltpu.VMEM((lanes, tile), bf16),
            pltpu.VMEM((2, owners, strip, tile), bf16),
            pltpu.VMEM((2, lanes, tile), f32),
            pltpu.VMEM((2, lanes, tile), f32),
            dma((slots,)),
            dma((len(counts), slots)),
            dma((slots,)),
            dma((2 * slots, 4)),
            dma((2 * slots, 4)),
            dma((2,)),
            dma((len(counts), slots)),
            dma((2,)),
            dma((dp,)),
            dma((dp,)),
            dma((3,)),
            dma((2,)),
            dma((2,)),
        ],
        compiler_params=pltpu.CompilerParams(
            collective_id=0, has_side_effects=True, vmem_limit_bytes=40 * 1024 * 1024
        ),
        cost_estimate=pl.CostEstimate(
            flops=8 * slots * lanes * tile * tile,
            bytes_accessed=slots * (12 * tile * tile + 20 * lanes * tile),
            transcendentals=0,
        ),
        name="exchange",
    )(sent, roots, left_roots, left_stats, right_stats)


def inner(partial_grads, owner_map, left_stats, right_stats, left_roots, right_roots):
    dp = lax.axis_size("dp")
    owners = lax.axis_size("owner")
    slots, lanes, tile = left_stats.shape[1:]
    if dp != 4 or owners % 2 or slots < 2:
        return general(
            partial_grads, owner_map, left_stats, right_stats, left_roots, right_roots
        )
    owner_here = lax.axis_index("owner")
    dp_here = lax.axis_index("dp")
    tiles = owner_map.shape[0]
    strip = lanes // owners
    rows, cols = extents(tiles)
    slot, tile_of, filled = owner_slots(owner_map, owners, slots)
    line = jnp.arange(strip, dtype=jnp.int32)
    wide_line = jnp.arange(tile, dtype=jnp.int32)
    shares = lax.psum_scatter(partial_grads[0], "dp", scatter_dimension=1, tiled=True)
    first = owner_here * (tile // owners) + dp_here * strip
    which = tile_of.reshape(-1)
    rows_of = jnp.where(filled.reshape(-1), jnp.take(rows, which), 0)
    cols_of = jnp.take(cols, which)
    keep = ((first + line)[None, :, None] < rows_of[:, None, None]) & (
        wide_line[None, None, :] < cols_of[:, None, None]
    )
    taken = jnp.take(shares, which, axis=0)
    sent = jnp.where(keep, taken, jnp.zeros((), taken.dtype))
    counts = (slots, slots)
    shape = (slots, owners, strip, tile)
    returned, new_left, new_right, _ = exchange(
        counts,
        sent.reshape(owners, slots, strip, tile),
        right_roots[0].reshape(shape),
        left_roots[0],
        left_stats[0],
        right_stats[0],
    )
    first = dp_here * lanes + owner_here * strip
    inside = ((first + line)[None, :, None] < rows[:, None, None]) & (
        wide_line[None, None, :] < cols[:, None, None]
    )
    flat = returned.reshape(owners * slots, strip, tile)
    direction = jnp.take(flat, owner_map * slots + slot, axis=0)
    direction = jnp.where(inside, direction, jnp.zeros((), direction.dtype))
    return (direction, new_left[None], new_right[None])


def solution(mesh):
    placed = (
        P("dp", None, "owner", None),
        P(),
        P("owner", None, "dp", None),
        P("owner", None, "dp", None),
        P("owner", None, "dp", None),
        P("owner", None, "dp", None),
    )
    return jax.shard_map(
        inner,
        mesh=mesh,
        in_specs=placed,
        out_specs=(
            P(None, ("dp", "owner"), None),
            P("owner", None, "dp", None),
            P("owner", None, "dp", None),
        ),
        check_vma=False,
    )
```

```python
import functools

import jax
import jax.numpy as jnp
from jax import lax
from jax.experimental import pallas as pl
from jax.experimental.pallas import tpu as pltpu
from jax.sharding import PartitionSpec as P


D_MODEL = 2560
D_IN = 10576
D_INNER = 5120
TILE = 1024

stat_decay = 0.999


def extents(count):
    index = jnp.arange(count, dtype=jnp.int32)
    in_cols = -(-D_IN // TILE)
    out_cols = -(-D_MODEL // TILE)
    in_count = -(-D_MODEL // TILE) * in_cols
    is_in = index < in_count
    other = jnp.maximum(index - in_count, 0)
    rows = jnp.where(
        is_in,
        jnp.minimum(TILE, D_MODEL - index // in_cols * TILE),
        jnp.minimum(TILE, D_INNER - other // out_cols * TILE),
    )
    cols = jnp.where(
        is_in,
        jnp.minimum(TILE, D_IN - index % in_cols * TILE),
        jnp.minimum(TILE, D_MODEL - other % out_cols * TILE),
    )
    return (rows, cols)


def dot(a, b, dims):
    return lax.dot_general(a, b, (dims, ((), ())), preferred_element_type=jnp.float32)


def step_kernel(base, info, grads, roots, left_roots, left_stats, right_stats, *rest):
    direction, new_left, new_right, left_part = rest[-4:]
    dp, _, _, piece, width = grads.shape
    lanes, tile = left_stats.shape[1:]
    here = info[0]
    pieces = lanes // piece
    full = [grads[d].reshape(tile, width) for d in range(dp)]
    mine = grads[here].reshape(tile, width).T
    gram = None
    for d in range(dp):
        right = dot(mine, full[d], ((1,), (0,)))
        cut = (0, slice(None), slice(d * width, (d + 1) * width))
        new_right[cut] = stat_decay * right_stats[cut] + (1.0 - stat_decay) * right
        part = dot(left_roots[0], full[d], ((1,), (0,)))
        left_part[:, d * width : (d + 1) * width] = part.astype(jnp.bfloat16)
        rows = grads[d, pl.ds(here * pieces, pieces)].reshape(lanes, width)
        term = dot(rows, full[d], ((1,), (1,)))
        gram = term if gram is None else gram + term
    new_left[0] = stat_decay * left_stats[0] + (1.0 - stat_decay) * gram
    product = dot(left_part[...], roots[...].reshape(tile, tile), ((1,), (0,)))
    slot = base + pl.program_id(0)
    row = lax.broadcasted_iota(jnp.int32, product.shape, 0)
    col = lax.broadcasted_iota(jnp.int32, product.shape, 1)
    keep = (row < info[1 + 2 * slot]) & (col < info[2 + 2 * slot])
    result = jnp.where(keep, product, 0.0).astype(jnp.bfloat16)
    direction[...] = result.reshape(direction.shape)


def step(base, chunk, info, grads, roots, left_roots, left_stats, right_stats, carried):
    dp, owners, _, piece, width = grads.shape
    _, lanes, tile = left_stats.shape
    at = lambda s, info: (base + s, 0, 0)
    stats = pl.BlockSpec((1, lanes, tile), at)
    in_specs = [
        pl.BlockSpec((dp, owners, 1, piece, width), lambda s, info: (0, 0, s, 0, 0)),
        pl.BlockSpec((dp, 1, lanes, tile), lambda s, info: (0, base + s, 0, 0)),
        stats,
        stats,
        stats,
    ] + [pl.BlockSpec(memory_space=pl.ANY)] * len(carried)
    sub = lanes // owners
    return pl.pallas_call(
        functools.partial(step_kernel, base),
        grid_spec=pltpu.PrefetchScalarGridSpec(
            num_scalar_prefetch=1,
            grid=(chunk,),
            in_specs=in_specs,
            out_specs=[
                pl.BlockSpec((owners, 1, sub, tile), lambda s, info: (0, s, 0, 0)),
                stats,
                stats,
            ],
            scratch_shapes=[pltpu.VMEM((lanes, tile), jnp.bfloat16)],
        ),
        out_shape=[
            jax.ShapeDtypeStruct((owners, chunk, sub, tile), jnp.bfloat16),
            jax.ShapeDtypeStruct(left_stats.shape, jnp.float32),
            jax.ShapeDtypeStruct(right_stats.shape, jnp.float32),
        ],
        input_output_aliases={6: 1, 7: 2} if carried else {},
        compiler_params=pltpu.CompilerParams(vmem_limit_bytes=48 * 1024 * 1024),
        cost_estimate=pl.CostEstimate(
            flops=8 * chunk * lanes * tile * tile,
            bytes_accessed=chunk * (4 * tile * tile + 20 * lanes * tile),
            transcendentals=0,
        ),
    )(info, grads, roots, left_roots, left_stats, right_stats, *carried)


def chunks_of(slots):
    if slots < 6:
        sizes = (slots,)
    else:
        last, middle = slots // 4, slots // 3
        sizes = (slots - middle - last, middle, last)
    return [(sum(sizes[:index]), size) for index, size in enumerate(sizes)]


def general(partial_grads, owner_map, left_stats, right_stats, left_roots, right_roots):
    dp = lax.axis_size("dp")
    owners = lax.axis_size("owner")
    owner_here = lax.axis_index("owner")
    dp_here = lax.axis_index("dp")
    tiles = owner_map.shape[0]
    slots = left_stats.shape[1]
    lanes = left_stats.shape[2]
    tile = left_stats.shape[3]
    piece = partial_grads.shape[2]
    width = tile // dp
    rows, cols = extents(tiles)
    ids = jnp.arange(tiles, dtype=jnp.int32)
    same = (owner_map[:, None] == owner_map[None, :]) & (ids[None, :] < ids[:, None])
    slot = jnp.sum(same.astype(jnp.int32), axis=1)
    picks = (slot[None, None, :] == jnp.arange(slots, dtype=jnp.int32)[None, :, None]) & (
        owner_map[None, None, :] == jnp.arange(owners, dtype=jnp.int32)[:, None, None]
    )
    tile_of = jnp.sum(jnp.where(picks, ids[None, None, :], 0), axis=2)
    filled = jnp.any(picks, axis=2)

    shares = lax.psum_scatter(partial_grads[0], "dp", scatter_dimension=2, tiled=True)
    roots = lax.all_gather(right_roots[0], "dp", axis=0)

    piece_rows = owner_here * piece + jnp.arange(piece, dtype=jnp.int32)
    piece_cols = dp_here * width + jnp.arange(width, dtype=jnp.int32)
    tile_here = lax.dynamic_index_in_dim(tile_of, owner_here, 0, keepdims=False)
    info = jnp.stack([jnp.take(rows, tile_here) - dp_here * lanes, jnp.take(cols, tile_here)], 1)
    info = jnp.concatenate([dp_here[None], info.reshape(-1)]).astype(jnp.int32)

    spans = chunks_of(slots)
    arrived = []
    for base, chunk in spans:
        which = tile_of[:, base : base + chunk]
        rows_of = jnp.where(filled[:, base : base + chunk], jnp.take(rows, which), 0)
        mask = (piece_rows[:, None] < rows_of[:, :, None, None]) & (
            piece_cols[None, :] < jnp.take(cols, which)[:, :, None, None]
        )
        taken = jnp.take(shares, which.reshape(-1), axis=0).reshape(owners, chunk, piece, width)
        sent = lax.all_to_all(
            jnp.where(mask, taken, jnp.zeros((), shares.dtype)),
            "owner",
            split_axis=0,
            concat_axis=0,
            tiled=True,
        )
        arrived.append(sent)

    def place(index, returned, direction):
        base, chunk = spans[index]
        flat = returned.reshape(owners * chunk, lanes // owners, tile)
        inside = (slot >= base) & (slot < base + chunk)
        at = jnp.where(inside, owner_map * chunk + slot - base, 0)
        return jnp.where(inside[:, None, None], jnp.take(flat, at, axis=0), direction)

    direction = jnp.zeros((tiles, lanes // owners, tile), jnp.bfloat16)
    carried = ()
    for index, (base, chunk) in enumerate(spans):
        grads = lax.all_gather(arrived[index], "dp", axis=0)
        if index:
            direction = place(index - 1, returned, direction)
            grads, direction = lax.optimization_barrier((grads, direction))
        result, *carried = step(
            base, chunk, info, grads, roots, left_roots[0], left_stats[0], right_stats[0], carried
        )
        returned = lax.all_to_all(result, "owner", split_axis=0, concat_axis=0, tiled=True)
    direction = place(len(spans) - 1, returned, direction)
    new_left, new_right = carried
    return (direction, new_left[None], new_right[None])


MESH = pl.DeviceIdType.MESH


def owner_slots(owner_map, owners, slots):
    tiles = owner_map.shape[0]
    ids = jnp.arange(tiles, dtype=jnp.int32)
    same = (owner_map[:, None] == owner_map[None, :]) & (ids[None, :] < ids[:, None])
    slot = jnp.sum(same.astype(jnp.int32), axis=1)
    picks = (slot[None, None, :] == jnp.arange(slots, dtype=jnp.int32)[None, :, None]) & (
        owner_map[None, None, :] == jnp.arange(owners, dtype=jnp.int32)[:, None, None]
    )
    tile_of = jnp.sum(jnp.where(picks, ids[None, None, :], 0), axis=2)
    return slot, tile_of, jnp.any(picks, axis=2)


def exchange_kernel(
    counts, sent, roots, left_roots, left_stats, right_stats,
    returned, new_left, new_right, wide,
    g_v, r_v, l_v, ls_v, rs_v, part_v, mine_v, out_v, nl_v, nr_v,
    own_sem, to_send, to_recv, wide_send, wide_recv, back_send, back_recv, back_own,
    g_sem, r_sem, in_sem, nl_sem, nr_sem,
):
    owners, slots, strip, tile = sent.shape
    lanes = left_roots.shape[1]
    parities = len(counts)
    panels = wide.shape[1]
    half = owners // 2
    pieces = lanes // (tile // owners)
    own = lax.axis_index("owner")
    me = lax.axis_index("dp")
    across = me + 1 - 2 * (me % 2)
    along = me + 2 - 4 * (me // 2)
    far = 3 - me
    kind = own % parities
    many = sum(jnp.where(kind == p, counts[p], 0) for p in range(parities))
    others = [(own + j) % owners for j in range(1, owners)]

    barrier = pltpu.get_barrier_semaphore()
    for peer in (across, along):
        pl.semaphore_signal(barrier, inc=1, device_id={"dp": peer}, device_id_type=MESH)
    for peer in others:
        pl.semaphore_signal(barrier, inc=1, device_id={"owner": peer}, device_id_type=MESH)
    pl.semaphore_wait(barrier, owners + 1)

    def each(low, high, act):
        lax.fori_loop(low, high, lambda i, c: (act(i), c)[1], 0)

    def place_of(item):
        return jnp.where(item < many, item, slots + item - many)

    def own_copy(s):
        return pltpu.make_async_copy(
            sent.at[own, s], wide.at[slots + s, me, own], own_sem.at[s]
        )

    def give(s, peer):
        return pltpu.make_async_remote_copy(
            src_ref=sent.at[peer, s],
            dst_ref=wide.at[slots + s, me, own],
            send_sem=to_send.at[peer % parities, s],
            recv_sem=to_recv.at[s],
            device_id={"owner": peer},
            device_id_type=MESH,
        )

    def direct(src, place, axis, peer):
        return pltpu.make_async_remote_copy(
            src_ref=src,
            dst_ref=wide.at[place, me],
            send_sem=wide_send.at[place, axis],
            recv_sem=wide_recv.at[place, axis],
            device_id={"dp": peer},
            device_id_type=MESH,
        )

    def forward(place, axis, panel, first, peer):
        piece = wide.at[place, panel, pl.ds(first, half)]
        return pltpu.make_async_remote_copy(
            src_ref=piece,
            dst_ref=piece,
            send_sem=wide_send.at[place, axis],
            recv_sem=wide_recv.at[place, axis],
            device_id={"dp": peer},
            device_id_type=MESH,
        )

    def sized(ref, sem):
        return pltpu.make_async_copy(ref, ref, sem)

    def loads(s):
        made = [pltpu.make_async_copy(roots.at[s], r_v.at[me], r_sem.at[0])]
        for index, panel in enumerate((across, along, far)):
            made.append(
                pltpu.make_async_copy(wide.at[s, panel], r_v.at[panel], r_sem.at[1 + index])
            )
        made.append(pltpu.make_async_copy(left_roots.at[s], l_v, in_sem.at[0]))
        made.append(pltpu.make_async_copy(left_stats.at[s], ls_v, in_sem.at[1]))
        made.append(pltpu.make_async_copy(right_stats.at[s], rs_v, in_sem.at[2]))
        return made

    def grads(s):
        return [
            pltpu.make_async_copy(wide.at[slots + s, j], g_v.at[:, j], g_sem.at[j])
            for j in range(panels)
        ]

    def back(s, side, peer):
        return pltpu.make_async_remote_copy(
            src_ref=out_v.at[side, peer],
            dst_ref=returned.at[own, s],
            send_sem=back_send.at[side],
            recv_sem=back_recv.at[kind, s],
            device_id={"owner": peer},
            device_id_type=MESH,
        )

    def back_home(s, side):
        return pltpu.make_async_copy(out_v.at[side, own], returned.at[own, s], back_own.at[side])

    def stats_out(s, side):
        return (
            pltpu.make_async_copy(nl_v.at[side], new_left.at[s], nl_sem.at[side]),
            pltpu.make_async_copy(nr_v.at[side], new_right.at[s], nr_sem.at[side]),
        )

    def settle(s, side):
        sized(returned.at[0, pl.ds(0, owners - 1)], back_send.at[side]).wait()
        back_home(s, side).wait()
        for copy in stats_out(s, side):
            copy.wait()

    width = lanes

    def compute(s):
        side = s % 2
        for copy in grads(s):
            copy.start()

        @pl.when(s == 0)
        def _():
            for copy in loads(0):
                copy.start()

        @pl.when(s >= 2)
        def _():
            settle(s - 2, side)

        for copy in grads(s) + loads(s):
            copy.wait()

        def cols(c):
            return pl.ds(pl.multiple_of(c * width, width), width)

        def column(c):
            return g_v[:, :, :, cols(c)].reshape(tile, width)

        def first(c):
            part = dot(l_v[...], column(c), ((1,), (0,)))
            part_v[:, cols(c)] = part.astype(jnp.bfloat16)

        def second(c):
            right = r_v[:, :, :, cols(c)].reshape(tile, width)
            product = dot(part_v[...], right, ((1,), (0,)))
            out_v[side, :, :, cols(c)] = product.astype(jnp.bfloat16).reshape(owners, strip, width)

        each(0, tile // width, first)
        each(0, tile // width, second)
        for peer in others:
            back(s, side, peer).start()
        back_home(s, side).start()
        mine_v[...] = column(me).T

        def third(c):
            right = dot(mine_v[...], column(c), ((1,), (0,)))
            nr_v[side, :, cols(c)] = stat_decay * rs_v[:, cols(c)] + (1.0 - stat_decay) * right
            rows = g_v[pl.ds(me * pieces, pieces)].reshape(lanes, tile)
            block = g_v[pl.ds(c * pieces, pieces)].reshape(lanes, tile)
            left = dot(rows, block, ((1,), (1,)))
            nl_v[side, :, cols(c)] = stat_decay * ls_v[:, cols(c)] + (1.0 - stat_decay) * left

        each(0, tile // width, third)
        for copy in stats_out(s, side):
            copy.start()

        @pl.when(s + 1 < many)
        def _():
            for copy in loads(s + 1):
                copy.start()

    each(0, many, lambda s: own_copy(s).start())

    def turn(i):
        @pl.when(i < many)
        def _():
            direct(roots.at[i], i, 0, across).start()
            direct(roots.at[i], i, 1, along).start()

        @pl.when(i < slots)
        def _():
            for peer in others:
                if min(counts) == slots:
                    give(i, peer).start()
                else:
                    for p in range(parities):
                        @pl.when((peer % parities == p) & (i < counts[p]))
                        def _():
                            give(i, peer).start()

        @pl.when((i >= many) & (i < 2 * many))
        def _():
            s = i - many
            own_copy(s).wait()
            sized(wide.at[slots + s, me, pl.ds(0, owners - 1)], to_recv.at[s]).wait()
            direct(wide.at[slots + s, me], slots + s, 0, across).start()
            direct(wide.at[slots + s, me], slots + s, 1, along).start()

        @pl.when((i >= 1) & (i < 2 * many + 1))
        def _():
            place = place_of(i - 1)
            sized(wide.at[place, across], wide_recv.at[place, 0]).wait()
            forward(place, 2, across, 0, along).start()
            sized(wide.at[place, along], wide_recv.at[place, 1]).wait()
            forward(place, 3, along, half, across).start()

        @pl.when(i >= 2)
        def _():
            place = place_of(i - 2)
            sized(wide.at[place, far, pl.ds(0, half)], wide_recv.at[place, 2]).wait()
            sized(wide.at[place, far, pl.ds(half, half)], wide_recv.at[place, 3]).wait()

        @pl.when(i >= many + 2)
        def _():
            compute(i - 2 - many)

    each(0, 2 * many + 2, turn)

    settle(many - 2, many % 2)
    settle(many - 1, (many + 1) % 2)

    if min(counts) < slots:
        def fade(s):
            moved = [
                pltpu.make_async_copy(left_stats.at[s], ls_v, in_sem.at[1]),
                pltpu.make_async_copy(right_stats.at[s], rs_v, in_sem.at[2]),
            ]
            for copy in moved:
                copy.start()
            for copy in moved:
                copy.wait()
            nl_v[0] = stat_decay * ls_v[...]
            nr_v[0] = stat_decay * rs_v[...]
            for copy in stats_out(s, 0):
                copy.start()
            for copy in stats_out(s, 0):
                copy.wait()

        each(many, slots, fade)

    def sends(item):
        place = place_of(item)
        panel = wide.at[place, me]
        part = wide.at[place, me, pl.ds(0, half)]
        sized(panel, wide_send.at[place, 0]).wait()
        sized(panel, wide_send.at[place, 1]).wait()
        sized(part, wide_send.at[place, 2]).wait()
        sized(part, wide_send.at[place, 3]).wait()

    each(0, 2 * many, sends)
    group = owners // parities
    for p in range(parities):
        def ends(s, p=p):
            for alike in (True, False):
                size = group - 1 if alike else group

                @pl.when((kind == p) == alike)
                def _():
                    piece = sent.at[0, pl.ds(0, size)]
                    sized(piece, to_send.at[p, s]).wait()
                    sized(piece, back_recv.at[p, s]).wait()

        each(0, counts[p], ends)


def exchange(index, counts, sent, roots, left_roots, left_stats, right_stats):
    owners, slots, strip, tile = sent.shape
    lanes = left_stats.shape[1]
    dp = tile // lanes
    anywhere = pl.BlockSpec(memory_space=pl.ANY)
    bf16, f32 = jnp.bfloat16, jnp.float32
    dma = pltpu.SemaphoreType.DMA
    return pl.pallas_call(
        functools.partial(exchange_kernel, counts),
        in_specs=[pl.BlockSpec(memory_space=pltpu.VMEM)] + [anywhere] * 4,
        out_specs=[anywhere] * 4,
        out_shape=[
            jax.ShapeDtypeStruct((owners, slots, strip, tile), bf16),
            jax.ShapeDtypeStruct(left_stats.shape, f32),
            jax.ShapeDtypeStruct(right_stats.shape, f32),
            jax.ShapeDtypeStruct((2 * slots, dp, owners, strip, tile), bf16),
        ],
        scratch_shapes=[
            pltpu.VMEM((owners, dp, strip, tile), bf16),
            pltpu.VMEM((dp, owners, strip, tile), bf16),
            pltpu.VMEM((lanes, tile), bf16),
            pltpu.VMEM((lanes, tile), f32),
            pltpu.VMEM((lanes, tile), f32),
            pltpu.VMEM((lanes, tile), bf16),
            pltpu.VMEM((lanes, tile), bf16),
            pltpu.VMEM((2, owners, strip, tile), bf16),
            pltpu.VMEM((2, lanes, tile), f32),
            pltpu.VMEM((2, lanes, tile), f32),
            dma((slots,)),
            dma((len(counts), slots)),
            dma((slots,)),
            dma((2 * slots, 4)),
            dma((2 * slots, 4)),
            dma((2,)),
            dma((len(counts), slots)),
            dma((2,)),
            dma((dp,)),
            dma((dp,)),
            dma((3,)),
            dma((2,)),
            dma((2,)),
        ],
        compiler_params=pltpu.CompilerParams(
            collective_id=index, has_side_effects=True, vmem_limit_bytes=40 * 1024 * 1024
        ),
        cost_estimate=pl.CostEstimate(
            flops=8 * slots * lanes * tile * tile,
            bytes_accessed=slots * (12 * tile * tile + 20 * lanes * tile),
            transcendentals=0,
        ),
    )(sent, roots, left_roots, left_stats, right_stats)[:3]


def inner(partial_grads, owner_map, left_stats, right_stats, left_roots, right_roots):
    dp = lax.axis_size("dp")
    owners = lax.axis_size("owner")
    slots, lanes, tile = left_stats.shape[1:]
    if dp != 4 or owners % 2 or slots < 2:
        return general(
            partial_grads, owner_map, left_stats, right_stats, left_roots, right_roots
        )
    owner_here = lax.axis_index("owner")
    dp_here = lax.axis_index("dp")
    tiles = owner_map.shape[0]
    strip = lanes // owners
    rows, cols = extents(tiles)
    slot, tile_of, filled = owner_slots(owner_map, owners, slots)
    line = jnp.arange(strip, dtype=jnp.int32)
    wide_line = jnp.arange(tile, dtype=jnp.int32)
    shares = lax.psum_scatter(partial_grads[0], "dp", scatter_dimension=1, tiled=True)
    first = owner_here * (tile // owners) + dp_here * strip
    which = tile_of.reshape(-1)
    rows_of = jnp.where(filled.reshape(-1), jnp.take(rows, which), 0)
    cols_of = jnp.take(cols, which)
    keep = ((first + line)[None, :, None] < rows_of[:, None, None]) & (
        wide_line[None, None, :] < cols_of[:, None, None]
    )
    taken = jnp.take(shares, which, axis=0)
    sent = jnp.where(keep, taken, jnp.zeros((), taken.dtype))
    held = jnp.sum(filled.astype(jnp.int32), axis=1).reshape(owners // 2, 2)
    most = jnp.max(held, axis=0)
    levels = [k for k in range(slots // 2, slots - 2) if 2 * k + 2 >= slots]
    plans = [(slots, slots)]
    for k in levels:
        plans += [(slots, k), (k, slots)]
    fewest = jnp.min(most)
    level = jnp.sum(jnp.array([fewest > k for k in levels]).astype(jnp.int32))
    plan = 1 + 2 * level + (most[0] < most[1]).astype(jnp.int32)
    plan = jnp.where(level == len(levels), 0, plan)
    shape = (slots, owners, strip, tile)
    returned, new_left, new_right = lax.switch(
        plan,
        [functools.partial(exchange, index, counts) for index, counts in enumerate(plans)],
        sent.reshape(owners, slots, strip, tile),
        right_roots[0].reshape(shape),
        left_roots[0],
        left_stats[0],
        right_stats[0],
    )
    first = dp_here * lanes + owner_here * strip
    inside = ((first + line)[None, :, None] < rows[:, None, None]) & (
        wide_line[None, None, :] < cols[:, None, None]
    )
    flat = returned.reshape(owners * slots, strip, tile)
    direction = jnp.take(flat, owner_map * slots + slot, axis=0)
    direction = jnp.where(inside, direction, jnp.zeros((), direction.dtype))
    return (direction, new_left[None], new_right[None])


def solution(mesh):
    placed = (
        P("dp", None, "owner", None),
        P(),
        P("owner", None, "dp", None),
        P("owner", None, "dp", None),
        P("owner", None, "dp", None),
        P("owner", None, "dp", None),
    )
    return jax.shard_map(
        inner,
        mesh=mesh,
        in_specs=placed,
        out_specs=(
            P(None, ("dp", "owner"), None),
            P("owner", None, "dp", None),
            P("owner", None, "dp", None),
        ),
        check_vma=False,
    )
```

```python
import functools

import jax
import jax.numpy as jnp
from jax import lax
from jax.experimental import pallas as pl
from jax.experimental.pallas import tpu as pltpu
from jax.sharding import PartitionSpec as P


D_MODEL = 2560
D_IN = 10576
D_INNER = 5120
TILE = 1024

stat_decay = 0.999


def extents(count):
    index = jnp.arange(count, dtype=jnp.int32)
    in_cols = -(-D_IN // TILE)
    out_cols = -(-D_MODEL // TILE)
    in_count = -(-D_MODEL // TILE) * in_cols
    is_in = index < in_count
    other = jnp.maximum(index - in_count, 0)
    rows = jnp.where(
        is_in,
        jnp.minimum(TILE, D_MODEL - index // in_cols * TILE),
        jnp.minimum(TILE, D_INNER - other // out_cols * TILE),
    )
    cols = jnp.where(
        is_in,
        jnp.minimum(TILE, D_IN - index % in_cols * TILE),
        jnp.minimum(TILE, D_MODEL - other % out_cols * TILE),
    )
    return (rows, cols)


def dot(a, b, dims):
    return lax.dot_general(a, b, (dims, ((), ())), preferred_element_type=jnp.float32)


def step_kernel(base, info, grads, roots, left_roots, left_stats, right_stats, *rest):
    direction, new_left, new_right, left_part = rest[-4:]
    dp, _, _, piece, width = grads.shape
    lanes, tile = left_stats.shape[1:]
    here = info[0]
    pieces = lanes // piece
    full = [grads[d].reshape(tile, width) for d in range(dp)]
    mine = grads[here].reshape(tile, width).T
    gram = None
    for d in range(dp):
        right = dot(mine, full[d], ((1,), (0,)))
        cut = (0, slice(None), slice(d * width, (d + 1) * width))
        new_right[cut] = stat_decay * right_stats[cut] + (1.0 - stat_decay) * right
        part = dot(left_roots[0], full[d], ((1,), (0,)))
        left_part[:, d * width : (d + 1) * width] = part.astype(jnp.bfloat16)
        rows = grads[d, pl.ds(here * pieces, pieces)].reshape(lanes, width)
        term = dot(rows, full[d], ((1,), (1,)))
        gram = term if gram is None else gram + term
    new_left[0] = stat_decay * left_stats[0] + (1.0 - stat_decay) * gram
    product = dot(left_part[...], roots[...].reshape(tile, tile), ((1,), (0,)))
    slot = base + pl.program_id(0)
    row = lax.broadcasted_iota(jnp.int32, product.shape, 0)
    col = lax.broadcasted_iota(jnp.int32, product.shape, 1)
    keep = (row < info[1 + 2 * slot]) & (col < info[2 + 2 * slot])
    result = jnp.where(keep, product, 0.0).astype(jnp.bfloat16)
    direction[...] = result.reshape(direction.shape)


def step(base, chunk, info, grads, roots, left_roots, left_stats, right_stats, carried):
    dp, owners, _, piece, width = grads.shape
    _, lanes, tile = left_stats.shape
    at = lambda s, info: (base + s, 0, 0)
    stats = pl.BlockSpec((1, lanes, tile), at)
    in_specs = [
        pl.BlockSpec((dp, owners, 1, piece, width), lambda s, info: (0, 0, s, 0, 0)),
        pl.BlockSpec((dp, 1, lanes, tile), lambda s, info: (0, base + s, 0, 0)),
        stats,
        stats,
        stats,
    ] + [pl.BlockSpec(memory_space=pl.ANY)] * len(carried)
    sub = lanes // owners
    return pl.pallas_call(
        functools.partial(step_kernel, base),
        grid_spec=pltpu.PrefetchScalarGridSpec(
            num_scalar_prefetch=1,
            grid=(chunk,),
            in_specs=in_specs,
            out_specs=[
                pl.BlockSpec((owners, 1, sub, tile), lambda s, info: (0, s, 0, 0)),
                stats,
                stats,
            ],
            scratch_shapes=[pltpu.VMEM((lanes, tile), jnp.bfloat16)],
        ),
        out_shape=[
            jax.ShapeDtypeStruct((owners, chunk, sub, tile), jnp.bfloat16),
            jax.ShapeDtypeStruct(left_stats.shape, jnp.float32),
            jax.ShapeDtypeStruct(right_stats.shape, jnp.float32),
        ],
        input_output_aliases={6: 1, 7: 2} if carried else {},
        compiler_params=pltpu.CompilerParams(vmem_limit_bytes=48 * 1024 * 1024),
        cost_estimate=pl.CostEstimate(
            flops=8 * chunk * lanes * tile * tile,
            bytes_accessed=chunk * (4 * tile * tile + 20 * lanes * tile),
            transcendentals=0,
        ),
    )(info, grads, roots, left_roots, left_stats, right_stats, *carried)


def chunks_of(slots):
    if slots < 6:
        sizes = (slots,)
    else:
        last, middle = slots // 4, slots // 3
        sizes = (slots - middle - last, middle, last)
    return [(sum(sizes[:index]), size) for index, size in enumerate(sizes)]


def general(partial_grads, owner_map, left_stats, right_stats, left_roots, right_roots):
    dp = lax.axis_size("dp")
    owners = lax.axis_size("owner")
    owner_here = lax.axis_index("owner")
    dp_here = lax.axis_index("dp")
    tiles = owner_map.shape[0]
    slots = left_stats.shape[1]
    lanes = left_stats.shape[2]
    tile = left_stats.shape[3]
    piece = partial_grads.shape[2]
    width = tile // dp
    rows, cols = extents(tiles)
    ids = jnp.arange(tiles, dtype=jnp.int32)
    same = (owner_map[:, None] == owner_map[None, :]) & (ids[None, :] < ids[:, None])
    slot = jnp.sum(same.astype(jnp.int32), axis=1)
    picks = (slot[None, None, :] == jnp.arange(slots, dtype=jnp.int32)[None, :, None]) & (
        owner_map[None, None, :] == jnp.arange(owners, dtype=jnp.int32)[:, None, None]
    )
    tile_of = jnp.sum(jnp.where(picks, ids[None, None, :], 0), axis=2)
    filled = jnp.any(picks, axis=2)

    shares = lax.psum_scatter(partial_grads[0], "dp", scatter_dimension=2, tiled=True)
    roots = lax.all_gather(right_roots[0], "dp", axis=0)

    piece_rows = owner_here * piece + jnp.arange(piece, dtype=jnp.int32)
    piece_cols = dp_here * width + jnp.arange(width, dtype=jnp.int32)
    tile_here = lax.dynamic_index_in_dim(tile_of, owner_here, 0, keepdims=False)
    info = jnp.stack([jnp.take(rows, tile_here) - dp_here * lanes, jnp.take(cols, tile_here)], 1)
    info = jnp.concatenate([dp_here[None], info.reshape(-1)]).astype(jnp.int32)

    spans = chunks_of(slots)
    arrived = []
    for base, chunk in spans:
        which = tile_of[:, base : base + chunk]
        rows_of = jnp.where(filled[:, base : base + chunk], jnp.take(rows, which), 0)
        mask = (piece_rows[:, None] < rows_of[:, :, None, None]) & (
            piece_cols[None, :] < jnp.take(cols, which)[:, :, None, None]
        )
        taken = jnp.take(shares, which.reshape(-1), axis=0).reshape(owners, chunk, piece, width)
        sent = lax.all_to_all(
            jnp.where(mask, taken, jnp.zeros((), shares.dtype)),
            "owner",
            split_axis=0,
            concat_axis=0,
            tiled=True,
        )
        arrived.append(sent)

    def place(index, returned, direction):
        base, chunk = spans[index]
        flat = returned.reshape(owners * chunk, lanes // owners, tile)
        inside = (slot >= base) & (slot < base + chunk)
        at = jnp.where(inside, owner_map * chunk + slot - base, 0)
        return jnp.where(inside[:, None, None], jnp.take(flat, at, axis=0), direction)

    direction = jnp.zeros((tiles, lanes // owners, tile), jnp.bfloat16)
    carried = ()
    for index, (base, chunk) in enumerate(spans):
        grads = lax.all_gather(arrived[index], "dp", axis=0)
        if index:
            direction = place(index - 1, returned, direction)
            grads, direction = lax.optimization_barrier((grads, direction))
        result, *carried = step(
            base, chunk, info, grads, roots, left_roots[0], left_stats[0], right_stats[0], carried
        )
        returned = lax.all_to_all(result, "owner", split_axis=0, concat_axis=0, tiled=True)
    direction = place(len(spans) - 1, returned, direction)
    new_left, new_right = carried
    return (direction, new_left[None], new_right[None])


MESH = pl.DeviceIdType.MESH


def index_kernel(levels, owner_map, tile_of, place, held, plan):
    tiles = owner_map.shape[0]
    owners = held.shape[0]
    slots = tile_of.shape[0] // owners

    def each(count, act):
        lax.fori_loop(0, count, lambda i, c: (act(i), c)[1], 0)

    def clear(q):
        tile_of[q] = tiles

    def empty(o):
        held[o] = 0

    def take(t):
        owner = owner_map[t]
        slot = held[owner]
        held[owner] = slot + 1
        place[t] = owner * slots + slot
        tile_of[owner * slots + slot] = t

    each(owners * slots, clear)
    each(owners, empty)
    each(tiles, take)
    most = [0, 0]
    for o in range(owners):
        most[o % 2] = jnp.maximum(most[o % 2], held[o])
    fewest = jnp.minimum(most[0], most[1])
    level = sum((fewest > k).astype(jnp.int32) for k in levels)
    choice = 1 + 2 * level + (most[0] < most[1]).astype(jnp.int32)
    plan[0] = jnp.where(level == len(levels), 0, choice)


def indices(owner_map, owners, slots, levels):
    tiles = owner_map.shape[0]
    scalars = pl.BlockSpec(memory_space=pltpu.SMEM)
    return pl.pallas_call(
        functools.partial(index_kernel, levels),
        in_specs=[scalars],
        out_specs=[scalars] * 4,
        out_shape=[
            jax.ShapeDtypeStruct((size,), jnp.int32) for size in (owners * slots, tiles, owners, 1)
        ],
        name="indices",
    )(owner_map)


def reduce_kernel(
    tile_of, rows, cols, partial, sent, mine_v, got_v, pass_v, last_v, shares_v,
    load_sem, send_sem, recv_sem, pass_send, pass_recv,
):
    pairs, _, batch, _, strip, tile = mine_v.shape
    owners, slots = sent.shape[:2]
    own = lax.axis_index("owner")
    me = lax.axis_index("dp")
    x, y = me % 2, me // 2
    across = me + 1 - 2 * x
    along = me + 2 - 4 * y
    peers = (across, along)
    barrier = pltpu.get_barrier_semaphore()
    for peer in peers:
        pl.semaphore_signal(barrier, inc=1, device_id={"dp": peer}, device_id_type=MESH)

    def each(count, act):
        lax.fori_loop(0, count, lambda i, c: (act(i), c)[1], 0)

    def blocks(p, way):
        return pl.ds((2 * p + way) * batch, batch)

    def load(p, way):
        part = partial.at[blocks(p, 0), :, x] if way == 0 else partial.at[blocks(p, 1), y]
        return pltpu.make_async_copy(part, mine_v.at[p, way], load_sem.at[p, way])

    def give(p, way):
        part = partial.at[blocks(p, 0), :, 1 - x] if way == 0 else partial.at[blocks(p, 1), 1 - y]
        return pltpu.make_async_remote_copy(
            src_ref=part,
            dst_ref=got_v.at[p, way],
            send_sem=send_sem.at[p, way],
            recv_sem=recv_sem.at[p, way],
            device_id={"dp": peers[way]},
            device_id_type=MESH,
        )

    def hand(p, way):
        return pltpu.make_async_remote_copy(
            src_ref=pass_v.at[p, way],
            dst_ref=last_v.at[p, way],
            send_sem=pass_send.at[p, way],
            recv_sem=pass_recv.at[p, way],
            device_id={"dp": peers[1 - way]},
            device_id_type=MESH,
        )

    def begin(p):
        for way in (0, 1):
            load(p, way).start()

    def offer(p):
        for way in (0, 1):
            give(p, way).start()

    def middle(p):
        for way in (0, 1):
            here = y if way == 0 else x
            load(p, way).wait()
            give(p, way).wait_recv()

            def add(b):
                total = mine_v[p, way, b, 1 - here].astype(jnp.float32)
                total = total + got_v[p, way, b, 1 - here].astype(jnp.float32)
                pass_v[p, way, b] = total.astype(jnp.bfloat16)

            each(batch, add)
            hand(p, way).start()

    def finish(p):
        for way in (0, 1):
            here = y if way == 0 else x
            hand(p, way).wait_recv()

            def add(b):
                t = (2 * p + way) * batch + b
                total = mine_v[p, way, b, here].astype(jnp.float32)
                total = total + got_v[p, way, b, here].astype(jnp.float32)
                total = total + last_v[p, way, b].astype(jnp.float32)
                first = own * (tile // owners) + me * strip
                row = first + lax.broadcasted_iota(jnp.int32, total.shape, 0)
                col = lax.broadcasted_iota(jnp.int32, total.shape, 1)
                keep = (row < rows[t]) & (col < cols[t])
                shares_v[t] = jnp.where(keep, total, 0.0).astype(jnp.bfloat16)

            each(batch, add)

    each(pairs, begin)
    pl.semaphore_wait(barrier, 2)
    each(pairs, offer)
    shares_v[2 * pairs * batch] = jnp.zeros((strip, tile), jnp.bfloat16)
    each(pairs, middle)
    each(pairs, finish)

    def fill(s):
        for o in range(owners):
            sent[o, s] = shares_v[tile_of[o * slots + s]]

    each(slots, fill)

    def ends(p):
        for way in (0, 1):
            give(p, way).wait_send()
            hand(p, way).wait_send()

    each(pairs, ends)


def reduce(tile_of, rows, cols, partial, owners, slots):
    tiles, _, _, strip, tile = partial.shape
    batch = 4
    pairs = tiles // (2 * batch)
    scalars = pl.BlockSpec(memory_space=pltpu.SMEM)
    bf16 = jnp.bfloat16
    dma = pltpu.SemaphoreType.DMA
    return pl.pallas_call(
        reduce_kernel,
        in_specs=[scalars] * 3 + [pl.BlockSpec(memory_space=pl.ANY)],
        out_specs=pl.BlockSpec(memory_space=pltpu.VMEM),
        out_shape=jax.ShapeDtypeStruct((owners, slots, strip, tile), bf16),
        scratch_shapes=[
            pltpu.VMEM((pairs, 2, batch, 2, strip, tile), bf16),
            pltpu.VMEM((pairs, 2, batch, 2, strip, tile), bf16),
            pltpu.VMEM((pairs, 2, batch, strip, tile), bf16),
            pltpu.VMEM((pairs, 2, batch, strip, tile), bf16),
            pltpu.VMEM((tiles + 1, strip, tile), bf16),
        ]
        + [dma((pairs, 2))] * 5,
        compiler_params=pltpu.CompilerParams(
            collective_id=0, has_side_effects=True, vmem_limit_bytes=48 * 1024 * 1024
        ),
        name="reduce",
    )(tile_of, rows, cols, partial)


def finish_kernel(place, rows, cols, held, *refs):
    batch = len(refs) - 7
    parts = refs[:batch]
    left_gram, right_gram, left_stats, right_stats, direction, new_left, new_right = refs[batch:]
    strip = direction.shape[1]
    lanes = left_stats.shape[1]
    own = lax.axis_index("owner")
    step = pl.program_id(0)
    filled = step < held[own]
    for gram, stats, new in (
        (left_gram, left_stats, new_left),
        (right_gram, right_stats, new_right),
    ):
        term = jnp.where(filled, gram[0].astype(jnp.float32), 0.0)
        new[0] = stat_decay * stats[0] + (1.0 - stat_decay) * term
    first = lax.axis_index("dp") * lanes + own * strip
    for b in range(batch):
        t = step * batch + b
        value = parts[b][0]
        row = first + lax.broadcasted_iota(jnp.int32, value.shape, 0)
        col = lax.broadcasted_iota(jnp.int32, value.shape, 1)
        keep = (row < rows[t]) & (col < cols[t])
        direction[b] = jnp.where(keep, value.astype(jnp.float32), 0.0).astype(jnp.bfloat16)


def finish(place, rows, cols, held, flat, left_gram, right_gram, left_stats, right_stats):
    slots, lanes, tile = left_stats.shape
    tiles = place.shape[0]
    strip = flat.shape[1]
    batch = tiles // slots
    part = lambda b: pl.BlockSpec(
        (1, strip, tile), lambda s, place, *rest: (place[s * batch + b], 0, 0)
    )
    block = pl.BlockSpec((1, lanes, tile), lambda s, *rest: (s, 0, 0))
    return pl.pallas_call(
        finish_kernel,
        grid_spec=pltpu.PrefetchScalarGridSpec(
            num_scalar_prefetch=4,
            grid=(slots,),
            in_specs=[part(b) for b in range(batch)] + [block] * 4,
            out_specs=[
                pl.BlockSpec((batch, strip, tile), lambda s, *rest: (s, 0, 0)),
                block,
                block,
            ],
        ),
        out_shape=[
            jax.ShapeDtypeStruct((tiles, strip, tile), jnp.bfloat16),
            jax.ShapeDtypeStruct(left_stats.shape, jnp.float32),
            jax.ShapeDtypeStruct(left_stats.shape, jnp.float32),
        ],
        compiler_params=pltpu.CompilerParams(vmem_limit_bytes=60 * 1024 * 1024),
        name="finish",
    )(place, rows, cols, held, *([flat] * batch), left_gram, right_gram, left_stats, right_stats)


def exchange_kernel(
    counts, sent, roots, left_roots,
    returned, left_gram, right_gram, wide,
    g_v, r_v, l_v, part_v, mine_v, out_v, nl_v, nr_v,
    own_sem, to_send, to_recv, wide_send, wide_recv, back_send, back_recv, back_own,
    g_sem, r_sem, in_sem, nl_sem, nr_sem,
):
    owners, slots, strip, tile = sent.shape
    lanes = left_roots.shape[1]
    parities = len(counts)
    panels = wide.shape[1]
    half = owners // 2
    pieces = lanes // (tile // owners)
    own = lax.axis_index("owner")
    me = lax.axis_index("dp")
    across = me + 1 - 2 * (me % 2)
    along = me + 2 - 4 * (me // 2)
    far = 3 - me
    kind = own % parities
    many = sum(jnp.where(kind == p, counts[p], 0) for p in range(parities))
    others = [(own + j) % owners for j in range(1, owners)]

    barrier = pltpu.get_barrier_semaphore()
    for peer in (across, along):
        pl.semaphore_signal(barrier, inc=1, device_id={"dp": peer}, device_id_type=MESH)
    for peer in others:
        pl.semaphore_signal(barrier, inc=1, device_id={"owner": peer}, device_id_type=MESH)
    pl.semaphore_wait(barrier, owners + 1)

    def each(low, high, act):
        lax.fori_loop(low, high, lambda i, c: (act(i), c)[1], 0)

    def place_of(item):
        return jnp.where(item < many, item, slots + item - many)

    def own_copy(s):
        return pltpu.make_async_copy(
            sent.at[own, s], wide.at[slots + s, me, own], own_sem.at[s]
        )

    def give(s, peer):
        return pltpu.make_async_remote_copy(
            src_ref=sent.at[peer, s],
            dst_ref=wide.at[slots + s, me, own],
            send_sem=to_send.at[peer % parities, s],
            recv_sem=to_recv.at[s],
            device_id={"owner": peer},
            device_id_type=MESH,
        )

    def direct(src, place, axis, peer):
        return pltpu.make_async_remote_copy(
            src_ref=src,
            dst_ref=wide.at[place, me],
            send_sem=wide_send.at[place, axis],
            recv_sem=wide_recv.at[place, axis],
            device_id={"dp": peer},
            device_id_type=MESH,
        )

    def forward(place, axis, panel, first, peer):
        piece = wide.at[place, panel, pl.ds(first, half)]
        return pltpu.make_async_remote_copy(
            src_ref=piece,
            dst_ref=piece,
            send_sem=wide_send.at[place, axis],
            recv_sem=wide_recv.at[place, axis],
            device_id={"dp": peer},
            device_id_type=MESH,
        )

    def sized(ref, sem):
        return pltpu.make_async_copy(ref, ref, sem)

    def loads(s):
        made = [pltpu.make_async_copy(roots.at[s], r_v.at[me], r_sem.at[0])]
        for index, panel in enumerate((across, along, far)):
            made.append(
                pltpu.make_async_copy(wide.at[s, panel], r_v.at[panel], r_sem.at[1 + index])
            )
        made.append(pltpu.make_async_copy(left_roots.at[s], l_v, in_sem.at[0]))
        return made

    def grads(s):
        return [
            pltpu.make_async_copy(wide.at[slots + s, j], g_v.at[:, j], g_sem.at[j])
            for j in range(panels)
        ]

    def back(s, side, peer):
        return pltpu.make_async_remote_copy(
            src_ref=out_v.at[side, peer],
            dst_ref=returned.at[own, s],
            send_sem=back_send.at[side],
            recv_sem=back_recv.at[kind, s],
            device_id={"owner": peer},
            device_id_type=MESH,
        )

    def back_home(s, side):
        return pltpu.make_async_copy(out_v.at[side, own], returned.at[own, s], back_own.at[side])

    def grams_out(s, side):
        return (
            pltpu.make_async_copy(nl_v.at[side], left_gram.at[s], nl_sem.at[side]),
            pltpu.make_async_copy(nr_v.at[side], right_gram.at[s], nr_sem.at[side]),
        )

    def settle(s, side):
        sized(returned.at[0, pl.ds(0, owners - 1)], back_send.at[side]).wait()
        back_home(s, side).wait()
        for copy in grams_out(s, side):
            copy.wait()

    width = lanes

    def compute(s):
        side = s % 2
        for copy in grads(s):
            copy.start()

        @pl.when(s == 0)
        def _():
            for copy in loads(0):
                copy.start()

        @pl.when(s >= 2)
        def _():
            settle(s - 2, side)

        for copy in grads(s) + loads(s):
            copy.wait()

        def cols(c):
            return pl.ds(pl.multiple_of(c * width, width), width)

        def column(c):
            return g_v[:, :, :, cols(c)].reshape(tile, width)

        def first(c):
            part = dot(l_v[...], column(c), ((1,), (0,)))
            part_v[:, cols(c)] = part.astype(jnp.bfloat16)

        def second(c):
            right = r_v[:, :, :, cols(c)].reshape(tile, width)
            product = dot(part_v[...], right, ((1,), (0,)))
            out_v[side, :, :, cols(c)] = product.astype(jnp.bfloat16).reshape(owners, strip, width)

        each(0, tile // width, first)
        each(0, tile // width, second)
        for peer in others:
            back(s, side, peer).start()
        back_home(s, side).start()
        mine_v[...] = column(me).T

        def third(c):
            right = dot(mine_v[...], column(c), ((1,), (0,)))
            nr_v[side, :, cols(c)] = right.astype(jnp.bfloat16)
            rows = g_v[pl.ds(me * pieces, pieces)].reshape(lanes, tile)
            block = g_v[pl.ds(c * pieces, pieces)].reshape(lanes, tile)
            left = dot(rows, block, ((1,), (1,)))
            nl_v[side, :, cols(c)] = left.astype(jnp.bfloat16)

        each(0, tile // width, third)
        for copy in grams_out(s, side):
            copy.start()

        @pl.when(s + 1 < many)
        def _():
            for copy in loads(s + 1):
                copy.start()

    each(0, many, lambda s: own_copy(s).start())

    def turn(i):
        @pl.when(i < many)
        def _():
            direct(roots.at[i], i, 0, across).start()
            direct(roots.at[i], i, 1, along).start()

        @pl.when(i < slots)
        def _():
            for peer in others:
                if min(counts) == slots:
                    give(i, peer).start()
                else:
                    for p in range(parities):
                        @pl.when((peer % parities == p) & (i < counts[p]))
                        def _():
                            give(i, peer).start()

        @pl.when((i >= many) & (i < 2 * many))
        def _():
            s = i - many
            own_copy(s).wait()
            sized(wide.at[slots + s, me, pl.ds(0, owners - 1)], to_recv.at[s]).wait()
            direct(wide.at[slots + s, me], slots + s, 0, across).start()
            direct(wide.at[slots + s, me], slots + s, 1, along).start()

        @pl.when((i >= 1) & (i < 2 * many + 1))
        def _():
            place = place_of(i - 1)
            sized(wide.at[place, across], wide_recv.at[place, 0]).wait()
            forward(place, 2, across, 0, along).start()
            sized(wide.at[place, along], wide_recv.at[place, 1]).wait()
            forward(place, 3, along, half, across).start()

        @pl.when(i >= 2)
        def _():
            place = place_of(i - 2)
            sized(wide.at[place, far, pl.ds(0, half)], wide_recv.at[place, 2]).wait()
            sized(wide.at[place, far, pl.ds(half, half)], wide_recv.at[place, 3]).wait()

        @pl.when(i >= many + 2)
        def _():
            compute(i - 2 - many)

    each(0, 2 * many + 2, turn)

    settle(many - 2, many % 2)
    settle(many - 1, (many + 1) % 2)

    def sends(item):
        place = place_of(item)
        panel = wide.at[place, me]
        part = wide.at[place, me, pl.ds(0, half)]
        sized(panel, wide_send.at[place, 0]).wait()
        sized(panel, wide_send.at[place, 1]).wait()
        sized(part, wide_send.at[place, 2]).wait()
        sized(part, wide_send.at[place, 3]).wait()

    each(0, 2 * many, sends)
    group = owners // parities
    for p in range(parities):
        def ends(s, p=p):
            for alike in (True, False):
                size = group - 1 if alike else group

                @pl.when((kind == p) == alike)
                def _():
                    piece = sent.at[0, pl.ds(0, size)]
                    sized(piece, to_send.at[p, s]).wait()
                    sized(piece, back_recv.at[p, s]).wait()

        each(0, counts[p], ends)


def exchange(index, counts, sent, roots, left_roots):
    owners, slots, strip, tile = sent.shape
    lanes = left_roots.shape[1]
    dp = tile // lanes
    anywhere = pl.BlockSpec(memory_space=pl.ANY)
    bf16 = jnp.bfloat16
    dma = pltpu.SemaphoreType.DMA
    return pl.pallas_call(
        functools.partial(exchange_kernel, counts),
        in_specs=[pl.BlockSpec(memory_space=pltpu.VMEM)] + [anywhere] * 2,
        out_specs=[anywhere] * 4,
        out_shape=[
            jax.ShapeDtypeStruct((owners, slots, strip, tile), bf16),
            jax.ShapeDtypeStruct(left_roots.shape, bf16),
            jax.ShapeDtypeStruct(left_roots.shape, bf16),
            jax.ShapeDtypeStruct((2 * slots, dp, owners, strip, tile), bf16),
        ],
        scratch_shapes=[
            pltpu.VMEM((owners, dp, strip, tile), bf16),
            pltpu.VMEM((dp, owners, strip, tile), bf16),
            pltpu.VMEM((lanes, tile), bf16),
            pltpu.VMEM((lanes, tile), bf16),
            pltpu.VMEM((lanes, tile), bf16),
            pltpu.VMEM((2, owners, strip, tile), bf16),
            pltpu.VMEM((2, lanes, tile), bf16),
            pltpu.VMEM((2, lanes, tile), bf16),
            dma((slots,)),
            dma((len(counts), slots)),
            dma((slots,)),
            dma((2 * slots, 4)),
            dma((2 * slots, 4)),
            dma((2,)),
            dma((len(counts), slots)),
            dma((2,)),
            dma((dp,)),
            dma((dp,)),
            dma((1,)),
            dma((2,)),
            dma((2,)),
        ],
        compiler_params=pltpu.CompilerParams(
            collective_id=1 + index, has_side_effects=True, vmem_limit_bytes=56 * 1024 * 1024
        ),
        cost_estimate=pl.CostEstimate(
            flops=8 * slots * lanes * tile * tile,
            bytes_accessed=slots * (12 * tile * tile + 20 * lanes * tile),
            transcendentals=0,
        ),
    )(sent, roots, left_roots)[:3]


def inner(partial_grads, owner_map, left_stats, right_stats, left_roots, right_roots):
    dp = lax.axis_size("dp")
    owners = lax.axis_size("owner")
    slots, lanes, tile = left_stats.shape[1:]
    tiles = owner_map.shape[0]
    if dp != 4 or owners % 2 or slots < 6 or tiles % slots or tiles % 8:
        return general(
            partial_grads, owner_map, left_stats, right_stats, left_roots, right_roots
        )
    strip = lanes // owners
    rows, cols = extents(tiles)
    levels = [k for k in range(slots // 2, slots - 2) if 2 * k + 2 >= slots]
    plans = [(slots, slots)]
    for k in levels:
        plans += [(slots, k), (k, slots)]
    tile_of, place, held, plan = indices(owner_map, owners, slots, levels)
    sent = reduce(
        tile_of, rows, cols, partial_grads[0].reshape(tiles, 2, 2, strip, tile), owners, slots
    )
    returned, left_gram, right_gram = lax.switch(
        plan[0],
        [functools.partial(exchange, index, counts) for index, counts in enumerate(plans)],
        sent,
        right_roots[0].reshape(slots, owners, strip, tile),
        left_roots[0],
    )
    direction, new_left, new_right = finish(
        place,
        rows,
        cols,
        held,
        returned.reshape(owners * slots, strip, tile),
        left_gram,
        right_gram,
        left_stats[0],
        right_stats[0],
    )
    return (direction, new_left[None], new_right[None])


def solution(mesh):
    placed = (
        P("dp", None, "owner", None),
        P(),
        P("owner", None, "dp", None),
        P("owner", None, "dp", None),
        P("owner", None, "dp", None),
        P("owner", None, "dp", None),
    )
    return jax.shard_map(
        inner,
        mesh=mesh,
        in_specs=placed,
        out_specs=(
            P(None, ("dp", "owner"), None),
            P("owner", None, "dp", None),
            P("owner", None, "dp", None),
        ),
        check_vma=False,
    )
```

```python
import functools

import jax
import jax.numpy as jnp
from jax import lax
from jax.experimental import pallas as pl
from jax.experimental.pallas import tpu as pltpu
from jax.sharding import PartitionSpec as P


D_MODEL = 2560
D_IN = 10576
D_INNER = 5120
TILE = 1024

stat_decay = 0.999


def extents(count):
    index = jnp.arange(count, dtype=jnp.int32)
    in_cols = -(-D_IN // TILE)
    out_cols = -(-D_MODEL // TILE)
    in_count = -(-D_MODEL // TILE) * in_cols
    is_in = index < in_count
    other = jnp.maximum(index - in_count, 0)
    rows = jnp.where(
        is_in,
        jnp.minimum(TILE, D_MODEL - index // in_cols * TILE),
        jnp.minimum(TILE, D_INNER - other // out_cols * TILE),
    )
    cols = jnp.where(
        is_in,
        jnp.minimum(TILE, D_IN - index % in_cols * TILE),
        jnp.minimum(TILE, D_MODEL - other % out_cols * TILE),
    )
    return (rows, cols)


def dot(a, b, dims):
    return lax.dot_general(a, b, (dims, ((), ())), preferred_element_type=jnp.float32)


def step_kernel(base, info, grads, roots, left_roots, left_stats, right_stats, *rest):
    direction, new_left, new_right, left_part = rest[-4:]
    dp, _, _, piece, width = grads.shape
    lanes, tile = left_stats.shape[1:]
    here = info[0]
    pieces = lanes // piece
    full = [grads[d].reshape(tile, width) for d in range(dp)]
    mine = grads[here].reshape(tile, width).T
    gram = None
    for d in range(dp):
        right = dot(mine, full[d], ((1,), (0,)))
        cut = (0, slice(None), slice(d * width, (d + 1) * width))
        new_right[cut] = stat_decay * right_stats[cut] + (1.0 - stat_decay) * right
        part = dot(left_roots[0], full[d], ((1,), (0,)))
        left_part[:, d * width : (d + 1) * width] = part.astype(jnp.bfloat16)
        rows = grads[d, pl.ds(here * pieces, pieces)].reshape(lanes, width)
        term = dot(rows, full[d], ((1,), (1,)))
        gram = term if gram is None else gram + term
    new_left[0] = stat_decay * left_stats[0] + (1.0 - stat_decay) * gram
    product = dot(left_part[...], roots[...].reshape(tile, tile), ((1,), (0,)))
    slot = base + pl.program_id(0)
    row = lax.broadcasted_iota(jnp.int32, product.shape, 0)
    col = lax.broadcasted_iota(jnp.int32, product.shape, 1)
    keep = (row < info[1 + 2 * slot]) & (col < info[2 + 2 * slot])
    result = jnp.where(keep, product, 0.0).astype(jnp.bfloat16)
    direction[...] = result.reshape(direction.shape)


def step(base, chunk, info, grads, roots, left_roots, left_stats, right_stats, carried):
    dp, owners, _, piece, width = grads.shape
    _, lanes, tile = left_stats.shape
    at = lambda s, info: (base + s, 0, 0)
    stats = pl.BlockSpec((1, lanes, tile), at)
    in_specs = [
        pl.BlockSpec((dp, owners, 1, piece, width), lambda s, info: (0, 0, s, 0, 0)),
        pl.BlockSpec((dp, 1, lanes, tile), lambda s, info: (0, base + s, 0, 0)),
        stats,
        stats,
        stats,
    ] + [pl.BlockSpec(memory_space=pl.ANY)] * len(carried)
    sub = lanes // owners
    return pl.pallas_call(
        functools.partial(step_kernel, base),
        grid_spec=pltpu.PrefetchScalarGridSpec(
            num_scalar_prefetch=1,
            grid=(chunk,),
            in_specs=in_specs,
            out_specs=[
                pl.BlockSpec((owners, 1, sub, tile), lambda s, info: (0, s, 0, 0)),
                stats,
                stats,
            ],
            scratch_shapes=[pltpu.VMEM((lanes, tile), jnp.bfloat16)],
        ),
        out_shape=[
            jax.ShapeDtypeStruct((owners, chunk, sub, tile), jnp.bfloat16),
            jax.ShapeDtypeStruct(left_stats.shape, jnp.float32),
            jax.ShapeDtypeStruct(right_stats.shape, jnp.float32),
        ],
        input_output_aliases={6: 1, 7: 2} if carried else {},
        compiler_params=pltpu.CompilerParams(vmem_limit_bytes=48 * 1024 * 1024),
        cost_estimate=pl.CostEstimate(
            flops=8 * chunk * lanes * tile * tile,
            bytes_accessed=chunk * (4 * tile * tile + 20 * lanes * tile),
            transcendentals=0,
        ),
    )(info, grads, roots, left_roots, left_stats, right_stats, *carried)


def chunks_of(slots):
    if slots < 6:
        sizes = (slots,)
    else:
        last, middle = slots // 4, slots // 3
        sizes = (slots - middle - last, middle, last)
    return [(sum(sizes[:index]), size) for index, size in enumerate(sizes)]


def general(partial_grads, owner_map, left_stats, right_stats, left_roots, right_roots):
    dp = lax.axis_size("dp")
    owners = lax.axis_size("owner")
    owner_here = lax.axis_index("owner")
    dp_here = lax.axis_index("dp")
    tiles = owner_map.shape[0]
    slots = left_stats.shape[1]
    lanes = left_stats.shape[2]
    tile = left_stats.shape[3]
    piece = partial_grads.shape[2]
    width = tile // dp
    rows, cols = extents(tiles)
    ids = jnp.arange(tiles, dtype=jnp.int32)
    same = (owner_map[:, None] == owner_map[None, :]) & (ids[None, :] < ids[:, None])
    slot = jnp.sum(same.astype(jnp.int32), axis=1)
    picks = (slot[None, None, :] == jnp.arange(slots, dtype=jnp.int32)[None, :, None]) & (
        owner_map[None, None, :] == jnp.arange(owners, dtype=jnp.int32)[:, None, None]
    )
    tile_of = jnp.sum(jnp.where(picks, ids[None, None, :], 0), axis=2)
    filled = jnp.any(picks, axis=2)

    shares = lax.psum_scatter(partial_grads[0], "dp", scatter_dimension=2, tiled=True)
    roots = lax.all_gather(right_roots[0], "dp", axis=0)

    piece_rows = owner_here * piece + jnp.arange(piece, dtype=jnp.int32)
    piece_cols = dp_here * width + jnp.arange(width, dtype=jnp.int32)
    tile_here = lax.dynamic_index_in_dim(tile_of, owner_here, 0, keepdims=False)
    info = jnp.stack([jnp.take(rows, tile_here) - dp_here * lanes, jnp.take(cols, tile_here)], 1)
    info = jnp.concatenate([dp_here[None], info.reshape(-1)]).astype(jnp.int32)

    spans = chunks_of(slots)
    arrived = []
    for base, chunk in spans:
        which = tile_of[:, base : base + chunk]
        rows_of = jnp.where(filled[:, base : base + chunk], jnp.take(rows, which), 0)
        mask = (piece_rows[:, None] < rows_of[:, :, None, None]) & (
            piece_cols[None, :] < jnp.take(cols, which)[:, :, None, None]
        )
        taken = jnp.take(shares, which.reshape(-1), axis=0).reshape(owners, chunk, piece, width)
        sent = lax.all_to_all(
            jnp.where(mask, taken, jnp.zeros((), shares.dtype)),
            "owner",
            split_axis=0,
            concat_axis=0,
            tiled=True,
        )
        arrived.append(sent)

    def place(index, returned, direction):
        base, chunk = spans[index]
        flat = returned.reshape(owners * chunk, lanes // owners, tile)
        inside = (slot >= base) & (slot < base + chunk)
        at = jnp.where(inside, owner_map * chunk + slot - base, 0)
        return jnp.where(inside[:, None, None], jnp.take(flat, at, axis=0), direction)

    direction = jnp.zeros((tiles, lanes // owners, tile), jnp.bfloat16)
    carried = ()
    for index, (base, chunk) in enumerate(spans):
        grads = lax.all_gather(arrived[index], "dp", axis=0)
        if index:
            direction = place(index - 1, returned, direction)
            grads, direction = lax.optimization_barrier((grads, direction))
        result, *carried = step(
            base, chunk, info, grads, roots, left_roots[0], left_stats[0], right_stats[0], carried
        )
        returned = lax.all_to_all(result, "owner", split_axis=0, concat_axis=0, tiled=True)
    direction = place(len(spans) - 1, returned, direction)
    new_left, new_right = carried
    return (direction, new_left[None], new_right[None])


MESH = pl.DeviceIdType.MESH


def index_kernel(levels, owner_map, tile_of, place, held, plan):
    tiles = owner_map.shape[0]
    owners = held.shape[0]
    slots = tile_of.shape[0] // owners

    def each(count, act):
        lax.fori_loop(0, count, lambda i, c: (act(i), c)[1], 0)

    def clear(q):
        tile_of[q] = tiles

    def empty(o):
        held[o] = 0

    def take(t):
        owner = owner_map[t]
        slot = held[owner]
        held[owner] = slot + 1
        place[t] = owner * slots + slot
        tile_of[owner * slots + slot] = t

    each(owners * slots, clear)
    each(owners, empty)
    each(tiles, take)
    most = [0, 0]
    for o in range(owners):
        most[o % 2] = jnp.maximum(most[o % 2], held[o])
    fewest = jnp.minimum(most[0], most[1])
    level = sum((fewest > k).astype(jnp.int32) for k in levels)
    choice = 1 + 2 * level + (most[0] < most[1]).astype(jnp.int32)
    plan[0] = jnp.where(level == len(levels), 0, choice)


def indices(owner_map, owners, slots, levels):
    tiles = owner_map.shape[0]
    scalars = pl.BlockSpec(memory_space=pltpu.SMEM)
    return pl.pallas_call(
        functools.partial(index_kernel, levels),
        in_specs=[scalars],
        out_specs=[scalars] * 4,
        out_shape=[
            jax.ShapeDtypeStruct((size,), jnp.int32) for size in (owners * slots, tiles, owners, 1)
        ],
        name="indices",
    )(owner_map)


def reduce_kernel(
    tile_of, rows, cols, partial, sent, mine_v, got_v, pass_v, last_v, shares_v,
    load_sem, send_sem, recv_sem, pass_send, pass_recv,
):
    pairs, _, batch, _, strip, tile = mine_v.shape
    owners, slots = sent.shape[:2]
    own = lax.axis_index("owner")
    me = lax.axis_index("dp")
    x, y = me % 2, me // 2
    across = me + 1 - 2 * x
    along = me + 2 - 4 * y
    peers = (across, along)
    barrier = pltpu.get_barrier_semaphore()
    for peer in peers:
        pl.semaphore_signal(barrier, inc=1, device_id={"dp": peer}, device_id_type=MESH)

    def each(count, act):
        lax.fori_loop(0, count, lambda i, c: (act(i), c)[1], 0)

    def blocks(p, way):
        return pl.ds((2 * p + way) * batch, batch)

    def load(p, way):
        part = partial.at[blocks(p, 0), :, x] if way == 0 else partial.at[blocks(p, 1), y]
        return pltpu.make_async_copy(part, mine_v.at[p, way], load_sem.at[p, way])

    def give(p, way):
        part = partial.at[blocks(p, 0), :, 1 - x] if way == 0 else partial.at[blocks(p, 1), 1 - y]
        return pltpu.make_async_remote_copy(
            src_ref=part,
            dst_ref=got_v.at[p, way],
            send_sem=send_sem.at[p, way],
            recv_sem=recv_sem.at[p, way],
            device_id={"dp": peers[way]},
            device_id_type=MESH,
        )

    def hand(p, way):
        return pltpu.make_async_remote_copy(
            src_ref=pass_v.at[p, way],
            dst_ref=last_v.at[p, way],
            send_sem=pass_send.at[p, way],
            recv_sem=pass_recv.at[p, way],
            device_id={"dp": peers[1 - way]},
            device_id_type=MESH,
        )

    def begin(p):
        for way in (0, 1):
            load(p, way).start()

    def offer(p):
        for way in (0, 1):
            give(p, way).start()

    def middle(p):
        for way in (0, 1):
            here = y if way == 0 else x
            load(p, way).wait()
            give(p, way).wait_recv()

            def add(b):
                total = mine_v[p, way, b, 1 - here].astype(jnp.float32)
                total = total + got_v[p, way, b, 1 - here].astype(jnp.float32)
                pass_v[p, way, b] = total.astype(jnp.bfloat16)

            each(batch, add)
            hand(p, way).start()

    def finish(p):
        for way in (0, 1):
            here = y if way == 0 else x
            hand(p, way).wait_recv()

            def add(b):
                t = (2 * p + way) * batch + b
                total = mine_v[p, way, b, here].astype(jnp.float32)
                total = total + got_v[p, way, b, here].astype(jnp.float32)
                total = total + last_v[p, way, b].astype(jnp.float32)
                first = own * (tile // owners) + me * strip
                row = first + lax.broadcasted_iota(jnp.int32, total.shape, 0)
                col = lax.broadcasted_iota(jnp.int32, total.shape, 1)
                keep = (row < rows[t]) & (col < cols[t])
                shares_v[t] = jnp.where(keep, total, 0.0).astype(jnp.bfloat16)

            each(batch, add)

    each(pairs, begin)
    pl.semaphore_wait(barrier, 2)
    each(pairs, offer)
    shares_v[2 * pairs * batch] = jnp.zeros((strip, tile), jnp.bfloat16)
    each(pairs, middle)
    each(pairs, finish)

    def fill(s):
        for o in range(owners):
            sent[o, s] = shares_v[tile_of[o * slots + s]]

    each(slots, fill)

    def ends(p):
        for way in (0, 1):
            give(p, way).wait_send()
            hand(p, way).wait_send()

    each(pairs, ends)


def reduce(tile_of, rows, cols, partial, owners, slots):
    tiles, _, _, strip, tile = partial.shape
    batch = 4
    pairs = tiles // (2 * batch)
    scalars = pl.BlockSpec(memory_space=pltpu.SMEM)
    bf16 = jnp.bfloat16
    dma = pltpu.SemaphoreType.DMA
    return pl.pallas_call(
        reduce_kernel,
        in_specs=[scalars] * 3 + [pl.BlockSpec(memory_space=pl.ANY)],
        out_specs=pl.BlockSpec(memory_space=pltpu.VMEM),
        out_shape=jax.ShapeDtypeStruct((owners, slots, strip, tile), bf16),
        scratch_shapes=[
            pltpu.VMEM((pairs, 2, batch, 2, strip, tile), bf16),
            pltpu.VMEM((pairs, 2, batch, 2, strip, tile), bf16),
            pltpu.VMEM((pairs, 2, batch, strip, tile), bf16),
            pltpu.VMEM((pairs, 2, batch, strip, tile), bf16),
            pltpu.VMEM((tiles + 1, strip, tile), bf16),
        ]
        + [dma((pairs, 2))] * 5,
        compiler_params=pltpu.CompilerParams(
            collective_id=0, has_side_effects=True, vmem_limit_bytes=48 * 1024 * 1024
        ),
        name="reduce",
    )(tile_of, rows, cols, partial)


def finish_kernel(
    place, rows, cols, flat, left, right, direction, new_left, new_right,
    held_v, left_sem, right_sem, in_sem, out_sem,
):
    tiles, strip, _ = held_v.shape
    slots, lanes = left.shape[:2]

    def each(count, act):
        lax.fori_loop(0, count, lambda i, c: (act(i), c)[1], 0)

    def bring(t):
        return pltpu.make_async_copy(flat.at[place[t]], held_v.at[t], in_sem.at[t])

    def put(t):
        return pltpu.make_async_copy(held_v.at[t], direction.at[t], out_sem.at[t])

    def store(s):
        return (
            pltpu.make_async_copy(left.at[s], new_left.at[s], left_sem.at[s]),
            pltpu.make_async_copy(right.at[s], new_right.at[s], right_sem.at[s]),
        )

    def start_all(s):
        for copy in store(s):
            copy.start()

    def wait_all(s):
        for copy in store(s):
            copy.wait()

    each(tiles, lambda t: bring(t).start())
    each(slots, start_all)
    first = lax.axis_index("dp") * lanes + lax.axis_index("owner") * strip

    def mask(t):
        bring(t).wait()
        value = held_v[t].astype(jnp.float32)
        row = first + lax.broadcasted_iota(jnp.int32, value.shape, 0)
        col = lax.broadcasted_iota(jnp.int32, value.shape, 1)
        keep = (row < rows[t]) & (col < cols[t])
        held_v[t] = jnp.where(keep, value, 0.0).astype(jnp.bfloat16)
        put(t).start()

    each(tiles, mask)
    each(tiles, lambda t: put(t).wait())
    each(slots, wait_all)


def finish(place, rows, cols, flat, left, right):
    slots, _, tile = left.shape
    tiles = place.shape[0]
    strip = flat.shape[1]
    scalars = pl.BlockSpec(memory_space=pltpu.SMEM)
    anywhere = pl.BlockSpec(memory_space=pltpu.HBM)
    near = pl.BlockSpec(memory_space=pltpu.VMEM)
    dma = pltpu.SemaphoreType.DMA
    return pl.pallas_call(
        finish_kernel,
        in_specs=[scalars] * 3 + [anywhere, near, near],
        out_specs=[anywhere] * 3,
        out_shape=[
            jax.ShapeDtypeStruct((tiles, strip, tile), jnp.bfloat16),
            jax.ShapeDtypeStruct(left.shape, jnp.float32),
            jax.ShapeDtypeStruct(left.shape, jnp.float32),
        ],
        scratch_shapes=[
            pltpu.VMEM((tiles, strip, tile), jnp.bfloat16),
            dma((slots,)),
            dma((slots,)),
            dma((tiles,)),
            dma((tiles,)),
        ],
        compiler_params=pltpu.CompilerParams(vmem_limit_bytes=8 * 1024 * 1024),
        name="finish",
    )(place, rows, cols, flat, left, right)


def exchange_kernel(
    counts, sent, roots, left_roots, left_stats, right_stats,
    returned, new_left, new_right, wide,
    g_v, r_v, l_v, part_v, mine_v, out_v,
    own_sem, to_send, to_recv, wide_send, wide_recv, back_send, back_recv, back_own,
    g_sem, r_sem, in_sem, left_sem, right_sem,
):
    owners, slots, strip, tile = sent.shape
    lanes = left_roots.shape[1]
    parities = len(counts)
    panels = wide.shape[1]
    half = owners // 2
    pieces = lanes // (tile // owners)
    own = lax.axis_index("owner")
    me = lax.axis_index("dp")
    across = me + 1 - 2 * (me % 2)
    along = me + 2 - 4 * (me // 2)
    far = 3 - me
    kind = own % parities
    many = sum(jnp.where(kind == p, counts[p], 0) for p in range(parities))
    others = [(own + j) % owners for j in range(1, owners)]

    barrier = pltpu.get_barrier_semaphore()
    for peer in (across, along):
        pl.semaphore_signal(barrier, inc=1, device_id={"dp": peer}, device_id_type=MESH)
    for peer in others:
        pl.semaphore_signal(barrier, inc=1, device_id={"owner": peer}, device_id_type=MESH)
    pl.semaphore_wait(barrier, owners + 1)

    def each(low, high, act):
        lax.fori_loop(low, high, lambda i, c: (act(i), c)[1], 0)

    lead = min(4, min(counts))

    def is_root(item):
        late = item - 2 * lead
        return (item < lead) | ((late >= 0) & (late % 2 == 1))

    def slot_of(item):
        late = lead + jnp.maximum(item - 2 * lead, 0) // 2
        return jnp.where(item < lead, item, jnp.where(item < 2 * lead, item - lead, late))

    def place_of(item):
        return jnp.where(is_root(item), 0, slots) + slot_of(item)

    def own_copy(s):
        return pltpu.make_async_copy(
            sent.at[own, s], wide.at[slots + s, me, own], own_sem.at[s]
        )

    def give(s, peer):
        return pltpu.make_async_remote_copy(
            src_ref=sent.at[peer, s],
            dst_ref=wide.at[slots + s, me, own],
            send_sem=to_send.at[peer % parities, s],
            recv_sem=to_recv.at[s],
            device_id={"owner": peer},
            device_id_type=MESH,
        )

    def direct(src, place, axis, peer):
        return pltpu.make_async_remote_copy(
            src_ref=src,
            dst_ref=wide.at[place, me],
            send_sem=wide_send.at[place, axis],
            recv_sem=wide_recv.at[place, axis],
            device_id={"dp": peer},
            device_id_type=MESH,
        )

    def forward(place, axis, panel, first, peer):
        piece = wide.at[place, panel, pl.ds(first, half)]
        return pltpu.make_async_remote_copy(
            src_ref=piece,
            dst_ref=piece,
            send_sem=wide_send.at[place, axis],
            recv_sem=wide_recv.at[place, axis],
            device_id={"dp": peer},
            device_id_type=MESH,
        )

    def sized(ref, sem):
        return pltpu.make_async_copy(ref, ref, sem)

    def root_loads(s):
        made = [pltpu.make_async_copy(roots.at[s], r_v.at[me], r_sem.at[0])]
        for index, panel in enumerate((across, along, far)):
            made.append(
                pltpu.make_async_copy(wide.at[s, panel], r_v.at[panel], r_sem.at[1 + index])
            )
        return made

    def left_load(s):
        return pltpu.make_async_copy(left_roots.at[s], l_v, in_sem.at[0])

    def stats_in(s):
        return (
            pltpu.make_async_copy(left_stats.at[s], new_left.at[s], left_sem.at[s]),
            pltpu.make_async_copy(right_stats.at[s], new_right.at[s], right_sem.at[s]),
        )

    def grads(s):
        return [
            pltpu.make_async_copy(wide.at[slots + s, j], g_v.at[:, j], g_sem.at[j])
            for j in range(panels)
        ]

    def back(s, side, peer):
        return pltpu.make_async_remote_copy(
            src_ref=out_v.at[side, peer],
            dst_ref=returned.at[own, s],
            send_sem=back_send.at[side],
            recv_sem=back_recv.at[kind, s],
            device_id={"owner": peer},
            device_id_type=MESH,
        )

    def back_home(s, side):
        return pltpu.make_async_copy(out_v.at[side, own], returned.at[own, s], back_own.at[side])

    def settle(side):
        sized(returned.at[0, pl.ds(0, owners - 1)], back_send.at[side]).wait()
        back_home(0, side).wait()

    width = lanes

    def cols(c):
        return pl.ds(pl.multiple_of(c * width, width), width)

    def column(c):
        return g_v[:, :, :, cols(c)].reshape(tile, width)

    def direct_part(s):
        side = s % 2

        @pl.when(s >= 2)
        def _():
            settle(side)

        for copy in root_loads(s):
            copy.wait()

        def act(c):
            right = r_v[:, :, :, cols(c)].reshape(tile, width)
            product = dot(part_v[...], right, ((1,), (0,)))
            out_v[side, :, :, cols(c)] = product.astype(jnp.bfloat16).reshape(owners, strip, width)

        each(0, tile // width, act)
        for peer in others:
            back(s, side, peer).start()
        back_home(s, side).start()

    def grads_part(s):
        for copy in grads(s):
            copy.start()

        @pl.when(s < lead)
        def _():
            for copy in root_loads(s):
                copy.start()

        left_load(s).wait()
        for copy in grads(s):
            copy.wait()

        def act(c):
            part = dot(l_v[...], column(c), ((1,), (0,)))
            part_v[:, cols(c)] = part.astype(jnp.bfloat16)

        each(0, tile // width, act)

        @pl.when(s + 1 < many)
        def _():
            left_load(s + 1).start()

        @pl.when(s < lead)
        def _():
            direct_part(s)

        for copy in stats_in(s):
            copy.wait()
        mine_v[...] = column(me).T

        def update(c):
            right = dot(mine_v[...], column(c), ((1,), (0,)))
            old = new_right[s, :, cols(c)]
            new_right[s, :, cols(c)] = stat_decay * old + (1.0 - stat_decay) * right
            rows = g_v[pl.ds(me * pieces, pieces)].reshape(lanes, tile)
            block = g_v[pl.ds(c * pieces, pieces)].reshape(lanes, tile)
            left = dot(rows, block, ((1,), (1,)))
            old = new_left[s, :, cols(c)]
            new_left[s, :, cols(c)] = stat_decay * old + (1.0 - stat_decay) * left

        each(0, tile // width, update)

    def begin(s):
        for copy in stats_in(s):
            copy.start()

    each(0, slots, begin)
    left_load(0).start()
    each(0, many, lambda s: own_copy(s).start())

    def turn(i):
        slot = slot_of(i)

        @pl.when((i < 2 * many) & is_root(i))
        def _():
            direct(roots.at[slot], slot, 0, across).start()
            direct(roots.at[slot], slot, 1, along).start()

        @pl.when(i < slots)
        def _():
            for peer in others:
                if min(counts) == slots:
                    give(i, peer).start()
                else:
                    for p in range(parities):
                        @pl.when((peer % parities == p) & (i < counts[p]))
                        def _():
                            give(i, peer).start()

        @pl.when((i < 2 * many) & jnp.logical_not(is_root(i)))
        def _():
            own_copy(slot).wait()
            sized(wide.at[slots + slot, me, pl.ds(0, owners - 1)], to_recv.at[slot]).wait()
            direct(wide.at[slots + slot, me], slots + slot, 0, across).start()
            direct(wide.at[slots + slot, me], slots + slot, 1, along).start()

        @pl.when((i >= 1) & (i < 2 * many + 1))
        def _():
            place = place_of(i - 1)
            sized(wide.at[place, across], wide_recv.at[place, 0]).wait()
            forward(place, 2, across, 0, along).start()
            sized(wide.at[place, along], wide_recv.at[place, 1]).wait()
            forward(place, 3, along, half, across).start()

        @pl.when(i >= 2)
        def _():
            place = place_of(i - 2)
            done = slot_of(i - 2)
            sized(wide.at[place, far, pl.ds(0, half)], wide_recv.at[place, 2]).wait()
            sized(wide.at[place, far, pl.ds(half, half)], wide_recv.at[place, 3]).wait()

            @pl.when(is_root(i - 2) & (done >= lead))
            def _():
                for copy in root_loads(done):
                    copy.start()
                direct_part(done)

            @pl.when(jnp.logical_not(is_root(i - 2)))
            def _():
                grads_part(done)

    each(0, 2 * many + 2, turn)

    settle(many % 2)
    settle((many + 1) % 2)

    if min(counts) < slots:
        def fade(s):
            for copy in stats_in(s):
                copy.wait()
            new_left[s] = stat_decay * new_left[s]
            new_right[s] = stat_decay * new_right[s]

        each(many, slots, fade)

    def sends(item):
        place = place_of(item)
        panel = wide.at[place, me]
        part = wide.at[place, me, pl.ds(0, half)]
        sized(panel, wide_send.at[place, 0]).wait()
        sized(panel, wide_send.at[place, 1]).wait()
        sized(part, wide_send.at[place, 2]).wait()
        sized(part, wide_send.at[place, 3]).wait()

    each(0, 2 * many, sends)
    group = owners // parities
    for p in range(parities):
        def ends(s, p=p):
            for alike in (True, False):
                size = group - 1 if alike else group

                @pl.when((kind == p) == alike)
                def _():
                    piece = sent.at[0, pl.ds(0, size)]
                    sized(piece, to_send.at[p, s]).wait()
                    sized(piece, back_recv.at[p, s]).wait()

        each(0, counts[p], ends)


def exchange(index, counts, sent, roots, left_roots, left_stats, right_stats):
    owners, slots, strip, tile = sent.shape
    lanes = left_roots.shape[1]
    dp = tile // lanes
    anywhere = pl.BlockSpec(memory_space=pltpu.HBM)
    near = pl.BlockSpec(memory_space=pltpu.VMEM)
    bf16 = jnp.bfloat16
    dma = pltpu.SemaphoreType.DMA
    return pl.pallas_call(
        functools.partial(exchange_kernel, counts),
        in_specs=[near] + [anywhere] * 4,
        out_specs=[anywhere, near, near, anywhere],
        out_shape=[
            jax.ShapeDtypeStruct((owners, slots, strip, tile), bf16),
            jax.ShapeDtypeStruct(left_stats.shape, jnp.float32),
            jax.ShapeDtypeStruct(left_stats.shape, jnp.float32),
            jax.ShapeDtypeStruct((2 * slots, dp, owners, strip, tile), bf16),
        ],
        scratch_shapes=[
            pltpu.VMEM((owners, dp, strip, tile), bf16),
            pltpu.VMEM((dp, owners, strip, tile), bf16),
            pltpu.VMEM((lanes, tile), bf16),
            pltpu.VMEM((lanes, tile), bf16),
            pltpu.VMEM((lanes, tile), bf16),
            pltpu.VMEM((2, owners, strip, tile), bf16),
            dma((slots,)),
            dma((len(counts), slots)),
            dma((slots,)),
            dma((2 * slots, 4)),
            dma((2 * slots, 4)),
            dma((2,)),
            dma((len(counts), slots)),
            dma((2,)),
            dma((dp,)),
            dma((dp,)),
            dma((1,)),
            dma((slots,)),
            dma((slots,)),
        ],
        compiler_params=pltpu.CompilerParams(
            collective_id=1 + index, has_side_effects=True, vmem_limit_bytes=16 * 1024 * 1024
        ),
        cost_estimate=pl.CostEstimate(
            flops=8 * slots * lanes * tile * tile,
            bytes_accessed=slots * (12 * tile * tile + 20 * lanes * tile),
            transcendentals=0,
        ),
    )(sent, roots, left_roots, left_stats, right_stats)[:3]


def inner(partial_grads, owner_map, left_stats, right_stats, left_roots, right_roots):
    dp = lax.axis_size("dp")
    owners = lax.axis_size("owner")
    slots, lanes, tile = left_stats.shape[1:]
    tiles = owner_map.shape[0]
    if dp != 4 or owners % 2 or slots < 6 or tiles % slots or tiles % 8:
        return general(
            partial_grads, owner_map, left_stats, right_stats, left_roots, right_roots
        )
    strip = lanes // owners
    rows, cols = extents(tiles)
    levels = [k for k in range(slots // 2, slots - 2) if 2 * k + 2 >= slots]
    plans = [(slots, slots)]
    for k in levels:
        plans += [(slots, k), (k, slots)]
    tile_of, place, _, plan = indices(owner_map, owners, slots, levels)
    sent = reduce(
        tile_of, rows, cols, partial_grads[0].reshape(tiles, 2, 2, strip, tile), owners, slots
    )

    def branch(index, counts):
        def run(place, rows, cols, *operands):
            returned, left, right = exchange(index, counts, *operands)
            flat = returned.reshape(owners * slots, strip, tile)
            return finish(place, rows, cols, flat, left, right)

        return run

    direction, new_left, new_right = lax.switch(
        plan[0],
        [branch(index, counts) for index, counts in enumerate(plans)],
        place,
        rows,
        cols,
        sent,
        right_roots[0].reshape(slots, owners, strip, tile),
        left_roots[0],
        left_stats[0],
        right_stats[0],
    )
    return (direction, new_left[None], new_right[None])


def solution(mesh):
    placed = (
        P("dp", None, "owner", None),
        P(),
        P("owner", None, "dp", None),
        P("owner", None, "dp", None),
        P("owner", None, "dp", None),
        P("owner", None, "dp", None),
    )
    return jax.shard_map(
        inner,
        mesh=mesh,
        in_specs=placed,
        out_specs=(
            P(None, ("dp", "owner"), None),
            P("owner", None, "dp", None),
            P("owner", None, "dp", None),
        ),
        check_vma=False,
    )
```

```python
import functools

import jax
import jax.numpy as jnp
from jax import lax
from jax.experimental import pallas as pl
from jax.experimental.pallas import tpu as pltpu
from jax.sharding import PartitionSpec as P


D_MODEL = 2560
D_IN = 10576
D_INNER = 5120
TILE = 1024

stat_decay = 0.999


def extents(count):
    return extents_at(jnp.arange(count, dtype=jnp.int32))


def extents_at(index):
    in_cols = -(-D_IN // TILE)
    out_cols = -(-D_MODEL // TILE)
    in_count = -(-D_MODEL // TILE) * in_cols
    is_in = index < in_count
    other = jnp.maximum(index - in_count, 0)
    rows = jnp.where(
        is_in,
        jnp.minimum(TILE, D_MODEL - index // in_cols * TILE),
        jnp.minimum(TILE, D_INNER - other // out_cols * TILE),
    )
    cols = jnp.where(
        is_in,
        jnp.minimum(TILE, D_IN - index % in_cols * TILE),
        jnp.minimum(TILE, D_MODEL - other % out_cols * TILE),
    )
    return (rows, cols)


def dot(a, b, dims):
    return lax.dot_general(a, b, (dims, ((), ())), preferred_element_type=jnp.float32)


def step_kernel(base, info, grads, roots, left_roots, left_stats, right_stats, *rest):
    direction, new_left, new_right, left_part = rest[-4:]
    dp, _, _, piece, width = grads.shape
    lanes, tile = left_stats.shape[1:]
    here = info[0]
    pieces = lanes // piece
    full = [grads[d].reshape(tile, width) for d in range(dp)]
    mine = grads[here].reshape(tile, width).T
    gram = None
    for d in range(dp):
        right = dot(mine, full[d], ((1,), (0,)))
        cut = (0, slice(None), slice(d * width, (d + 1) * width))
        new_right[cut] = stat_decay * right_stats[cut] + (1.0 - stat_decay) * right
        part = dot(left_roots[0], full[d], ((1,), (0,)))
        left_part[:, d * width : (d + 1) * width] = part.astype(jnp.bfloat16)
        rows = grads[d, pl.ds(here * pieces, pieces)].reshape(lanes, width)
        term = dot(rows, full[d], ((1,), (1,)))
        gram = term if gram is None else gram + term
    new_left[0] = stat_decay * left_stats[0] + (1.0 - stat_decay) * gram
    product = dot(left_part[...], roots[...].reshape(tile, tile), ((1,), (0,)))
    slot = base + pl.program_id(0)
    row = lax.broadcasted_iota(jnp.int32, product.shape, 0)
    col = lax.broadcasted_iota(jnp.int32, product.shape, 1)
    keep = (row < info[1 + 2 * slot]) & (col < info[2 + 2 * slot])
    result = jnp.where(keep, product, 0.0).astype(jnp.bfloat16)
    direction[...] = result.reshape(direction.shape)


def step(base, chunk, info, grads, roots, left_roots, left_stats, right_stats, carried):
    dp, owners, _, piece, width = grads.shape
    _, lanes, tile = left_stats.shape
    at = lambda s, info: (base + s, 0, 0)
    stats = pl.BlockSpec((1, lanes, tile), at)
    in_specs = [
        pl.BlockSpec((dp, owners, 1, piece, width), lambda s, info: (0, 0, s, 0, 0)),
        pl.BlockSpec((dp, 1, lanes, tile), lambda s, info: (0, base + s, 0, 0)),
        stats,
        stats,
        stats,
    ] + [pl.BlockSpec(memory_space=pl.ANY)] * len(carried)
    sub = lanes // owners
    return pl.pallas_call(
        functools.partial(step_kernel, base),
        grid_spec=pltpu.PrefetchScalarGridSpec(
            num_scalar_prefetch=1,
            grid=(chunk,),
            in_specs=in_specs,
            out_specs=[
                pl.BlockSpec((owners, 1, sub, tile), lambda s, info: (0, s, 0, 0)),
                stats,
                stats,
            ],
            scratch_shapes=[pltpu.VMEM((lanes, tile), jnp.bfloat16)],
        ),
        out_shape=[
            jax.ShapeDtypeStruct((owners, chunk, sub, tile), jnp.bfloat16),
            jax.ShapeDtypeStruct(left_stats.shape, jnp.float32),
            jax.ShapeDtypeStruct(right_stats.shape, jnp.float32),
        ],
        input_output_aliases={6: 1, 7: 2} if carried else {},
        compiler_params=pltpu.CompilerParams(vmem_limit_bytes=48 * 1024 * 1024),
        cost_estimate=pl.CostEstimate(
            flops=8 * chunk * lanes * tile * tile,
            bytes_accessed=chunk * (4 * tile * tile + 20 * lanes * tile),
            transcendentals=0,
        ),
    )(info, grads, roots, left_roots, left_stats, right_stats, *carried)


def chunks_of(slots):
    if slots < 6:
        sizes = (slots,)
    else:
        last, middle = slots // 4, slots // 3
        sizes = (slots - middle - last, middle, last)
    return [(sum(sizes[:index]), size) for index, size in enumerate(sizes)]


def general(partial_grads, owner_map, left_stats, right_stats, left_roots, right_roots):
    dp = lax.axis_size("dp")
    owners = lax.axis_size("owner")
    owner_here = lax.axis_index("owner")
    dp_here = lax.axis_index("dp")
    tiles = owner_map.shape[0]
    slots = left_stats.shape[1]
    lanes = left_stats.shape[2]
    tile = left_stats.shape[3]
    piece = partial_grads.shape[2]
    width = tile // dp
    rows, cols = extents(tiles)
    ids = jnp.arange(tiles, dtype=jnp.int32)
    same = (owner_map[:, None] == owner_map[None, :]) & (ids[None, :] < ids[:, None])
    slot = jnp.sum(same.astype(jnp.int32), axis=1)
    picks = (slot[None, None, :] == jnp.arange(slots, dtype=jnp.int32)[None, :, None]) & (
        owner_map[None, None, :] == jnp.arange(owners, dtype=jnp.int32)[:, None, None]
    )
    tile_of = jnp.sum(jnp.where(picks, ids[None, None, :], 0), axis=2)
    filled = jnp.any(picks, axis=2)

    shares = lax.psum_scatter(partial_grads[0], "dp", scatter_dimension=2, tiled=True)
    roots = lax.all_gather(right_roots[0], "dp", axis=0)

    piece_rows = owner_here * piece + jnp.arange(piece, dtype=jnp.int32)
    piece_cols = dp_here * width + jnp.arange(width, dtype=jnp.int32)
    tile_here = lax.dynamic_index_in_dim(tile_of, owner_here, 0, keepdims=False)
    info = jnp.stack([jnp.take(rows, tile_here) - dp_here * lanes, jnp.take(cols, tile_here)], 1)
    info = jnp.concatenate([dp_here[None], info.reshape(-1)]).astype(jnp.int32)

    spans = chunks_of(slots)
    arrived = []
    for base, chunk in spans:
        which = tile_of[:, base : base + chunk]
        rows_of = jnp.where(filled[:, base : base + chunk], jnp.take(rows, which), 0)
        mask = (piece_rows[:, None] < rows_of[:, :, None, None]) & (
            piece_cols[None, :] < jnp.take(cols, which)[:, :, None, None]
        )
        taken = jnp.take(shares, which.reshape(-1), axis=0).reshape(owners, chunk, piece, width)
        sent = lax.all_to_all(
            jnp.where(mask, taken, jnp.zeros((), shares.dtype)),
            "owner",
            split_axis=0,
            concat_axis=0,
            tiled=True,
        )
        arrived.append(sent)

    def place(index, returned, direction):
        base, chunk = spans[index]
        flat = returned.reshape(owners * chunk, lanes // owners, tile)
        inside = (slot >= base) & (slot < base + chunk)
        at = jnp.where(inside, owner_map * chunk + slot - base, 0)
        return jnp.where(inside[:, None, None], jnp.take(flat, at, axis=0), direction)

    direction = jnp.zeros((tiles, lanes // owners, tile), jnp.bfloat16)
    carried = ()
    for index, (base, chunk) in enumerate(spans):
        grads = lax.all_gather(arrived[index], "dp", axis=0)
        if index:
            direction = place(index - 1, returned, direction)
            grads, direction = lax.optimization_barrier((grads, direction))
        result, *carried = step(
            base, chunk, info, grads, roots, left_roots[0], left_stats[0], right_stats[0], carried
        )
        returned = lax.all_to_all(result, "owner", split_axis=0, concat_axis=0, tiled=True)
    direction = place(len(spans) - 1, returned, direction)
    new_left, new_right = carried
    return (direction, new_left[None], new_right[None])


MESH = pl.DeviceIdType.MESH


def index_kernel(levels, side_slots, rest_slots, owner_map, tile_of, place, held, plan):
    tiles = owner_map.shape[0]
    owners = held.shape[0]
    slots = tile_of.shape[0] // owners

    def each(count, act):
        lax.fori_loop(0, count, lambda i, c: (act(i), c)[1], 0)

    def clear(q):
        tile_of[q] = tiles

    def empty(o):
        held[o] = 0

    def take(t):
        owner = owner_map[t]
        slot = held[owner]
        held[owner] = slot + 1
        place[t] = owner * slots + slot
        tile_of[owner * slots + slot] = t

    each(owners * slots, clear)
    each(owners, empty)
    each(tiles, take)
    most = [0, 0]
    for o in range(owners):
        most[o % 2] = jnp.maximum(most[o % 2], held[o])
    fewest = jnp.minimum(most[0], most[1])
    level = sum((fewest > k).astype(jnp.int32) for k in levels)
    choice = 1 + 2 * level + (most[0] < most[1]).astype(jnp.int32)
    choice = jnp.where(level == len(levels), 0, choice)
    for o in range(owners):
        mate = o + 1 - 2 * (o % 2)
        others = [held[q] for q in range(owners) if q not in (o, mate)]
        fits = (held[mate] <= side_slots) & (functools.reduce(jnp.maximum, others) <= rest_slots)
        choice = jnp.where(fits, 1 + 2 * len(levels) + o, choice)
    plan[0] = choice


def indices(owner_map, owners, slots, levels, side_slots, rest_slots):
    tiles = owner_map.shape[0]
    scalars = pl.BlockSpec(memory_space=pltpu.SMEM)
    return pl.pallas_call(
        functools.partial(index_kernel, levels, side_slots, rest_slots),
        in_specs=[scalars],
        out_specs=[scalars] * 4,
        out_shape=[
            jax.ShapeDtypeStruct((size,), jnp.int32) for size in (owners * slots, tiles, owners, 1)
        ],
        name="indices",
    )(owner_map)


def reduce_kernel(
    tile_of, rows, cols, partial, sent, mine_v, got_v, pass_v, last_v, shares_v,
    load_sem, send_sem, recv_sem, pass_send, pass_recv,
):
    pairs, _, batch, _, strip, tile = mine_v.shape
    owners, slots = sent.shape[:2]
    own = lax.axis_index("owner")
    me = lax.axis_index("dp")
    x, y = me % 2, me // 2
    across = me + 1 - 2 * x
    along = me + 2 - 4 * y
    peers = (across, along)
    barrier = pltpu.get_barrier_semaphore()
    for peer in peers:
        pl.semaphore_signal(barrier, inc=1, device_id={"dp": peer}, device_id_type=MESH)

    def each(count, act):
        lax.fori_loop(0, count, lambda i, c: (act(i), c)[1], 0)

    def blocks(p, way):
        return pl.ds((2 * p + way) * batch, batch)

    def load(p, way):
        part = partial.at[blocks(p, 0), :, x] if way == 0 else partial.at[blocks(p, 1), y]
        return pltpu.make_async_copy(part, mine_v.at[p, way], load_sem.at[p, way])

    def give(p, way):
        part = partial.at[blocks(p, 0), :, 1 - x] if way == 0 else partial.at[blocks(p, 1), 1 - y]
        return pltpu.make_async_remote_copy(
            src_ref=part,
            dst_ref=got_v.at[p, way],
            send_sem=send_sem.at[p, way],
            recv_sem=recv_sem.at[p, way],
            device_id={"dp": peers[way]},
            device_id_type=MESH,
        )

    def hand(p, way):
        return pltpu.make_async_remote_copy(
            src_ref=pass_v.at[p, way],
            dst_ref=last_v.at[p, way],
            send_sem=pass_send.at[p, way],
            recv_sem=pass_recv.at[p, way],
            device_id={"dp": peers[1 - way]},
            device_id_type=MESH,
        )

    def begin(p):
        for way in (0, 1):
            load(p, way).start()

    def offer(p):
        for way in (0, 1):
            give(p, way).start()

    def middle(p):
        for way in (0, 1):
            here = y if way == 0 else x
            load(p, way).wait()
            give(p, way).wait_recv()

            def add(b):
                total = mine_v[p, way, b, 1 - here].astype(jnp.float32)
                total = total + got_v[p, way, b, 1 - here].astype(jnp.float32)
                pass_v[p, way, b] = total.astype(jnp.bfloat16)

            each(batch, add)
            hand(p, way).start()

    def finish(p):
        for way in (0, 1):
            here = y if way == 0 else x
            hand(p, way).wait_recv()

            def add(b):
                t = (2 * p + way) * batch + b
                total = mine_v[p, way, b, here].astype(jnp.float32)
                total = total + got_v[p, way, b, here].astype(jnp.float32)
                total = total + last_v[p, way, b].astype(jnp.float32)
                first = own * (tile // owners) + me * strip
                row = first + lax.broadcasted_iota(jnp.int32, total.shape, 0)
                col = lax.broadcasted_iota(jnp.int32, total.shape, 1)
                keep = (row < rows[t]) & (col < cols[t])
                shares_v[t] = jnp.where(keep, total, 0.0).astype(jnp.bfloat16)

            each(batch, add)

    each(pairs, begin)
    pl.semaphore_wait(barrier, 2)
    each(pairs, offer)
    shares_v[2 * pairs * batch] = jnp.zeros((strip, tile), jnp.bfloat16)
    each(pairs, middle)
    each(pairs, finish)

    def fill(s):
        for o in range(owners):
            sent[o, s] = shares_v[tile_of[o * slots + s]]

    each(slots, fill)

    def ends(p):
        for way in (0, 1):
            give(p, way).wait_send()
            hand(p, way).wait_send()

    each(pairs, ends)


def reduce(tile_of, rows, cols, partial, owners, slots):
    tiles, _, _, strip, tile = partial.shape
    batch = 4
    pairs = tiles // (2 * batch)
    scalars = pl.BlockSpec(memory_space=pltpu.SMEM)
    bf16 = jnp.bfloat16
    dma = pltpu.SemaphoreType.DMA
    return pl.pallas_call(
        reduce_kernel,
        in_specs=[scalars] * 3 + [pl.BlockSpec(memory_space=pl.ANY)],
        out_specs=pl.BlockSpec(memory_space=pltpu.VMEM),
        out_shape=jax.ShapeDtypeStruct((owners, slots, strip, tile), bf16),
        scratch_shapes=[
            pltpu.VMEM((pairs, 2, batch, 2, strip, tile), bf16),
            pltpu.VMEM((pairs, 2, batch, 2, strip, tile), bf16),
            pltpu.VMEM((pairs, 2, batch, strip, tile), bf16),
            pltpu.VMEM((pairs, 2, batch, strip, tile), bf16),
            pltpu.VMEM((tiles + 1, strip, tile), bf16),
        ]
        + [dma((pairs, 2))] * 5,
        compiler_params=pltpu.CompilerParams(
            collective_id=0, has_side_effects=True, vmem_limit_bytes=48 * 1024 * 1024
        ),
        name="reduce",
    )(tile_of, rows, cols, partial)


def finish_kernel(
    place, flat, left, right, direction, new_left, new_right, held_v, left_sem, right_sem, out_sem
):
    tiles, strip, _ = held_v.shape
    slots, lanes = left.shape[:2]

    def each(count, act):
        lax.fori_loop(0, count, lambda i, c: (act(i), c)[1], 0)

    def put(t):
        return pltpu.make_async_copy(held_v.at[t], direction.at[t], out_sem.at[t])

    def store(s):
        return (
            pltpu.make_async_copy(left.at[s], new_left.at[s], left_sem.at[s]),
            pltpu.make_async_copy(right.at[s], new_right.at[s], right_sem.at[s]),
        )

    def start_all(s):
        for copy in store(s):
            copy.start()

    def wait_all(s):
        for copy in store(s):
            copy.wait()

    each(slots, start_all)
    first = lax.axis_index("dp") * lanes + lax.axis_index("owner") * strip

    def mask(t):
        rows, cols = extents_at(t)
        value = flat[place[t]].astype(jnp.float32)
        row = first + lax.broadcasted_iota(jnp.int32, value.shape, 0)
        col = lax.broadcasted_iota(jnp.int32, value.shape, 1)
        keep = (row < rows) & (col < cols)
        held_v[t] = jnp.where(keep, value, 0.0).astype(jnp.bfloat16)
        put(t).start()

    each(tiles, mask)
    each(tiles, lambda t: put(t).wait())
    each(slots, wait_all)


def finish(place, flat, left, right):
    slots, _, tile = left.shape
    tiles = place.shape[0]
    strip = flat.shape[1]
    anywhere = pl.BlockSpec(memory_space=pl.ANY)
    near = pl.BlockSpec(memory_space=pltpu.VMEM)
    dma = pltpu.SemaphoreType.DMA
    return pl.pallas_call(
        finish_kernel,
        in_specs=[pl.BlockSpec(memory_space=pltpu.SMEM), near, near, near],
        out_specs=[anywhere] * 3,
        out_shape=[
            jax.ShapeDtypeStruct((tiles, strip, tile), jnp.bfloat16),
            jax.ShapeDtypeStruct(left.shape, jnp.float32),
            jax.ShapeDtypeStruct(left.shape, jnp.float32),
        ],
        scratch_shapes=[
            pltpu.VMEM((tiles, strip, tile), jnp.bfloat16),
            dma((slots,)),
            dma((slots,)),
            dma((tiles,)),
        ],
        compiler_params=pltpu.CompilerParams(vmem_limit_bytes=8 * 1024 * 1024),
        name="finish",
    )(place, flat, left, right)


def exchange_kernel(
    groups, sent, roots, left_roots, left_stats, right_stats,
    returned, new_left, new_right, wide,
    g_v, r_v, l_v, part_v, mine_v, out_v,
    own_sem, to_send, to_recv, wide_send, wide_recv, back_send, back_recv,
    g_sem, r_sem, in_sem, left_sem, right_sem,
):
    owners, slots, strip, tile = sent.shape
    lanes = left_roots.shape[1]
    counts = [count for count, _ in groups]
    panels = wide.shape[1]
    half = owners // 2
    pieces = lanes // (tile // owners)
    own = lax.axis_index("owner")
    me = lax.axis_index("dp")
    across = me + 1 - 2 * (me % 2)
    along = me + 2 - 4 * (me // 2)
    far = 3 - me

    def group_of(owner):
        return sum(
            jnp.where(owner == member, g, 0)
            for g, (_, members) in enumerate(groups)
            for member in members
        )

    def count_of(group):
        return sum(jnp.where(group == g, count, 0) for g, count in enumerate(counts))

    kind = group_of(own)
    many = count_of(kind)

    barrier = pltpu.get_barrier_semaphore()
    for peer in (across, along):
        pl.semaphore_signal(barrier, inc=1, device_id={"dp": peer}, device_id_type=MESH)

    def each(low, high, act):
        lax.fori_loop(low, high, lambda i, c: (act(i), c)[1], 0)

    def others(act):
        each(1, owners, lambda j: act((own + j) % owners))

    def greet(peer):
        pl.semaphore_signal(barrier, inc=1, device_id={"owner": peer}, device_id_type=MESH)

    others(greet)
    pl.semaphore_wait(barrier, owners + 1)

    lead = min(4, min(counts))

    def is_root(item):
        late = item - 2 * lead
        return (item < lead) | ((late >= 0) & (late % 2 == 1))

    def slot_of(item):
        late = lead + jnp.maximum(item - 2 * lead, 0) // 2
        return jnp.where(item < lead, item, jnp.where(item < 2 * lead, item - lead, late))

    def place_of(item):
        return jnp.where(is_root(item), 0, slots) + slot_of(item)

    def own_copy(s):
        return pltpu.make_async_copy(
            sent.at[own, s], wide.at[slots + s, me, own], own_sem.at[s]
        )

    def give(s, peer, group):
        return pltpu.make_async_remote_copy(
            src_ref=sent.at[peer, s],
            dst_ref=wide.at[slots + s, me, own],
            send_sem=to_send.at[group, s],
            recv_sem=to_recv.at[s],
            device_id={"owner": peer},
            device_id_type=MESH,
        )

    def direct(src, place, axis, peer):
        return pltpu.make_async_remote_copy(
            src_ref=src,
            dst_ref=wide.at[place, me],
            send_sem=wide_send.at[place, axis],
            recv_sem=wide_recv.at[place, axis],
            device_id={"dp": peer},
            device_id_type=MESH,
        )

    def forward(place, axis, panel, first, peer):
        piece = wide.at[place, panel, pl.ds(first, half)]
        return pltpu.make_async_remote_copy(
            src_ref=piece,
            dst_ref=piece,
            send_sem=wide_send.at[place, axis],
            recv_sem=wide_recv.at[place, axis],
            device_id={"dp": peer},
            device_id_type=MESH,
        )

    def sized(ref, sem):
        return pltpu.make_async_copy(ref, ref, sem)

    def root_loads(s):
        made = [pltpu.make_async_copy(roots.at[s], r_v.at[me], r_sem.at[0])]
        for index, panel in enumerate((across, along, far)):
            made.append(
                pltpu.make_async_copy(wide.at[s, panel], r_v.at[panel], r_sem.at[1 + index])
            )
        return made

    def left_load(s):
        return pltpu.make_async_copy(left_roots.at[s], l_v, in_sem.at[0])

    def stats_in(s):
        return (
            pltpu.make_async_copy(left_stats.at[s], new_left.at[s], left_sem.at[s]),
            pltpu.make_async_copy(right_stats.at[s], new_right.at[s], right_sem.at[s]),
        )

    def grads(s):
        return [
            pltpu.make_async_copy(wide.at[slots + s, j], g_v.at[:, j], g_sem.at[j])
            for j in range(panels)
        ]

    def back(s, side, peer):
        return pltpu.make_async_remote_copy(
            src_ref=out_v.at[side, peer],
            dst_ref=returned.at[own, s],
            send_sem=back_send.at[side],
            recv_sem=back_recv.at[kind, s],
            device_id={"owner": peer},
            device_id_type=MESH,
        )

    def settle(side):
        sized(sent.at[0, pl.ds(0, owners - 1)], back_send.at[side]).wait()

    width = lanes

    def cols(c):
        return pl.ds(pl.multiple_of(c * width, width), width)

    def column(c):
        return g_v[:, :, :, cols(c)].reshape(tile, width)

    def arrive(s, root_too):
        for copy in grads(s):
            copy.start()

        @pl.when(root_too)
        def _():
            for copy in root_loads(s):
                copy.start()

        left_load(s).wait()
        for copy in grads(s):
            copy.wait()

        def act(c):
            part = dot(l_v[...], column(c), ((1,), (0,)))
            part_v[:, cols(c)] = part.astype(jnp.bfloat16)

        each(0, tile // width, act)

        @pl.when(s + 1 < many)
        def _():
            left_load(s + 1).start()

    def direction(s):
        side = s % 2

        @pl.when(s >= 2)
        def _():
            settle(side)

        for copy in root_loads(s):
            copy.wait()

        def act(c):
            right = r_v[:, :, :, cols(c)].reshape(tile, width)
            product = dot(part_v[...], right, ((1,), (0,)))
            out_v[side, :, :, cols(c)] = product.astype(jnp.bfloat16).reshape(owners, strip, width)

        each(0, tile // width, act)
        others(lambda peer: back(s, side, peer).start())
        returned[own, s] = out_v[side, own]

    def statistics(s):
        for copy in stats_in(s):
            copy.wait()

        def turned(c):
            block = g_v[pl.ds(c * pieces, pieces), :, :, cols(me)].reshape(lanes, width)
            mine_v[:, cols(c)] = block.T

        each(0, tile // width, turned)

        def update(c):
            right = dot(mine_v[...], column(c), ((1,), (0,)))
            old = new_right[s, :, cols(c)]
            new_right[s, :, cols(c)] = stat_decay * old + (1.0 - stat_decay) * right
            rows = g_v[pl.ds(me * pieces, pieces)].reshape(lanes, tile)
            block = g_v[pl.ds(c * pieces, pieces)].reshape(lanes, tile)
            left = dot(rows, block, ((1,), (1,)))
            old = new_left[s, :, cols(c)]
            new_left[s, :, cols(c)] = stat_decay * old + (1.0 - stat_decay) * left

        each(0, tile // width, update)

    def begin(s):
        for copy in stats_in(s):
            copy.start()

    left_load(0).start()
    each(0, many, lambda s: own_copy(s).start())

    def turn(i):
        slot = slot_of(i)

        @pl.when((i < 2 * many) & is_root(i))
        def _():
            direct(roots.at[slot], slot, 0, across).start()
            direct(roots.at[slot], slot, 1, along).start()

        def offer(peer):
            group = group_of(peer)

            @pl.when(i < count_of(group))
            def _():
                give(i, peer, group).start()

        @pl.when(i < slots)
        def _():
            others(offer)
            begin(i)

        @pl.when((i < 2 * many) & jnp.logical_not(is_root(i)))
        def _():
            own_copy(slot).wait()
            sized(wide.at[slots + slot, me, pl.ds(0, owners - 1)], to_recv.at[slot]).wait()
            direct(wide.at[slots + slot, me], slots + slot, 0, across).start()
            direct(wide.at[slots + slot, me], slots + slot, 1, along).start()

        @pl.when((i >= 1) & (i < 2 * many + 1))
        def _():
            place = place_of(i - 1)
            sized(wide.at[place, across], wide_recv.at[place, 0]).wait()
            forward(place, 2, across, 0, along).start()
            sized(wide.at[place, along], wide_recv.at[place, 1]).wait()
            forward(place, 3, along, half, across).start()

        @pl.when(i >= 2)
        def _():
            place = place_of(i - 2)
            done = slot_of(i - 2)
            sized(wide.at[place, far, pl.ds(0, half)], wide_recv.at[place, 2]).wait()
            sized(wide.at[place, far, pl.ds(half, half)], wide_recv.at[place, 3]).wait()

            root = is_root(i - 2)
            early = done < lead

            @pl.when(root & jnp.logical_not(early))
            def _():
                for copy in root_loads(done):
                    copy.start()

            @pl.when(jnp.logical_not(root))
            def _():
                arrive(done, early)

            @pl.when(root != early)
            def _():
                direction(done)

            @pl.when(jnp.logical_not(root))
            def _():
                statistics(done)

    each(0, 2 * many + 2, turn)

    settle(many % 2)
    settle((many + 1) % 2)

    if min(counts) < slots:
        def fade(s):
            for copy in stats_in(s):
                copy.wait()
            new_left[s] = stat_decay * new_left[s]
            new_right[s] = stat_decay * new_right[s]

        each(many, slots, fade)

    def sends(item):
        place = place_of(item)
        panel = wide.at[place, me]
        part = wide.at[place, me, pl.ds(0, half)]
        sized(panel, wide_send.at[place, 0]).wait()
        sized(panel, wide_send.at[place, 1]).wait()
        sized(part, wide_send.at[place, 2]).wait()
        sized(part, wide_send.at[place, 3]).wait()

    each(0, 2 * many, sends)
    for g, (count, members) in enumerate(groups):
        def ends(s, g=g, members=members):
            for alike in (True, False):
                size = len(members) - 1 if alike else len(members)
                if size:
                    @pl.when((kind == g) == alike)
                    def _():
                        piece = sent.at[0, pl.ds(0, size)]
                        sized(piece, to_send.at[g, s]).wait()
                        sized(piece, back_recv.at[g, s]).wait()

        each(0, count, ends)


def exchange(index, groups, sent, roots, left_roots, left_stats, right_stats):
    owners, slots, strip, tile = sent.shape
    lanes = left_roots.shape[1]
    dp = tile // lanes
    anywhere = pl.BlockSpec(memory_space=pltpu.HBM)
    near = pl.BlockSpec(memory_space=pltpu.VMEM)
    bf16 = jnp.bfloat16
    dma = pltpu.SemaphoreType.DMA
    return pl.pallas_call(
        functools.partial(exchange_kernel, groups),
        in_specs=[near] + [anywhere] * 4,
        out_specs=[near, near, near, anywhere],
        out_shape=[
            jax.ShapeDtypeStruct((owners, slots, strip, tile), bf16),
            jax.ShapeDtypeStruct(left_stats.shape, jnp.float32),
            jax.ShapeDtypeStruct(left_stats.shape, jnp.float32),
            jax.ShapeDtypeStruct((2 * slots, dp, owners, strip, tile), bf16),
        ],
        scratch_shapes=[
            pltpu.VMEM((owners, dp, strip, tile), bf16),
            pltpu.VMEM((dp, owners, strip, tile), bf16),
            pltpu.VMEM((lanes, tile), bf16),
            pltpu.VMEM((lanes, tile), bf16),
            pltpu.VMEM((lanes, tile), bf16),
            pltpu.VMEM((2, owners, strip, tile), bf16),
            dma((slots,)),
            dma((len(groups), slots)),
            dma((slots,)),
            dma((2 * slots, 4)),
            dma((2 * slots, 4)),
            dma((2,)),
            dma((len(groups), slots)),
            dma((dp,)),
            dma((dp,)),
            dma((1,)),
            dma((slots,)),
            dma((slots,)),
        ],
        compiler_params=pltpu.CompilerParams(
            collective_id=1 + index, has_side_effects=True, vmem_limit_bytes=16 * 1024 * 1024
        ),
        cost_estimate=pl.CostEstimate(
            flops=8 * slots * lanes * tile * tile,
            bytes_accessed=slots * (12 * tile * tile + 20 * lanes * tile),
            transcendentals=0,
        ),
    )(sent, roots, left_roots, left_stats, right_stats)[:3]


def inner(partial_grads, owner_map, left_stats, right_stats, left_roots, right_roots):
    dp = lax.axis_size("dp")
    owners = lax.axis_size("owner")
    slots, lanes, tile = left_stats.shape[1:]
    tiles = owner_map.shape[0]
    if dp != 4 or owners % 2 or slots < 6 or tiles % slots or tiles % 8:
        return general(
            partial_grads, owner_map, left_stats, right_stats, left_roots, right_roots
        )
    strip = lanes // owners
    levels = [k for k in range(slots // 2 + 1, slots - 2) if 2 * k + 2 >= slots]
    side_slots = -(-slots // 2) - 1
    rest_slots = (slots + side_slots) // 2
    evens, odds = range(0, owners, 2), range(1, owners, 2)
    plans = [((slots, evens), (slots, odds))]
    for k in levels:
        plans += [((slots, evens), (k, odds)), ((k, evens), (slots, odds))]
    for o in range(owners):
        mate = o + 1 - 2 * (o % 2)
        rest = [q for q in range(owners) if q not in (o, mate)]
        plans.append(((slots, (o,)), (side_slots, (mate,)), (rest_slots, rest)))
    tile_of, place, _, plan = indices(owner_map, owners, slots, levels, side_slots, rest_slots)
    rows, cols = extents(tiles)
    sent = reduce(
        tile_of, rows, cols, partial_grads[0].reshape(tiles, 2, 2, strip, tile), owners, slots
    )

    def branch(index, groups):
        def run(place, *operands):
            returned, left, right = exchange(index, groups, *operands)
            return finish(place, returned.reshape(owners * slots, strip, tile), left, right)

        return run

    direction, new_left, new_right = lax.switch(
        plan[0],
        [branch(index, groups) for index, groups in enumerate(plans)],
        place,
        sent,
        right_roots[0].reshape(slots, owners, strip, tile),
        left_roots[0],
        left_stats[0],
        right_stats[0],
    )
    return (direction, new_left[None], new_right[None])


def solution(mesh):
    placed = (
        P("dp", None, "owner", None),
        P(),
        P("owner", None, "dp", None),
        P("owner", None, "dp", None),
        P("owner", None, "dp", None),
        P("owner", None, "dp", None),
    )
    return jax.shard_map(
        inner,
        mesh=mesh,
        in_specs=placed,
        out_specs=(
            P(None, ("dp", "owner"), None),
            P("owner", None, "dp", None),
            P("owner", None, "dp", None),
        ),
        check_vma=False,
    )
```
